128 devices in a mesh: member: 16 (over x_lo, y, core), strip: 8 (over z, x_hi).
Axes of the slice: x: 4 (x_hi: 2, x_lo: 2; x = x_hi * 2 + x_lo), y: 4, z: 4, core: 2. Of those that a mesh axis runs over, the one named last changes fastest.
Arguments:
- sample_fields: float32 [64, 3, 128, 2048], P('member', None, 'strip'), may hold values from -0.8 to 0.8
- report_counts: int32 [8, 16], P('strip', 'member'), may hold values from 1 to 256, as said below
- report_cells: int32 [8, 16, 256], P('strip', 'member'), may hold values from 0 to 2047
- report_values: float32 [8, 16, 256], P('strip', 'member'), may hold values from -1.5 to 1.5
- report_errors: float32 [8, 16, 256], P('strip', 'member'), may hold values from 0.04 to 0.2
- local_radius: int32 [8, 16], P('strip', 'member'), may hold values from 1 to 3
Outputs:
- analysis: float32 [64, 3, 128, 2048], P('member', None, 'strip')
The draws below stay inside these ranges and needn't reach their ends.
Inputs may be any that keep to these rules, and one draw needn't show every extreme that they name: `report_counts`: counts lie between 1 and 256; 256 is reached by some region in every draw; slots from the count on are not used.
All inputs are finite; a program needn't handle non-finite values.
Results may differ from the reference program's by a relative error of at most 0.0003.
Values sent between devices are 32-bit elements; how exact they have to be, the bound alone decides.
A program may use at most 64 MiB of HBM per device.

```python
import math
import jax
import jax.numpy as jnp
from jax import lax

MEMBERS = 64
BAND_HEIGHT_CELLS = 16
PATCH_WIDTH_CELLS = 128
OBS_MAX = 256
STEPS = 12
TURNS = 20
NORTHWARD_PATCHES = 8
EASTWARD_PATCHES = 16
NX = 128
NY = 2048


def draw_report_counts(key, part):
    key_shift, key_trim, key_pick = jax.random.split(jax.random.fold_in(key, 7), 3)
    grid_shape = (NORTHWARD_PATCHES, EASTWARD_PATCHES)
    shifts = jax.random.randint(key_shift, grid_shape, 0, 4)
    trimmed = jax.random.randint(key_trim, grid_shape, 0, OBS_MAX // 8 + 1)
    counts = jnp.maximum(jnp.right_shift(jnp.int32(OBS_MAX), shifts) - trimmed, 1)
    chosen = jax.random.randint(key_pick, (), 0, NORTHWARD_PATCHES * EASTWARD_PATCHES)
    flattened = counts.reshape(-1)
    flattened = jnp.where(jnp.arange(NORTHWARD_PATCHES * EASTWARD_PATCHES) == chosen, OBS_MAX, flattened)
    return flattened.reshape(grid_shape).astype(jnp.int32)


def with_ends(result, own_key, least, high):
    spot = [jax.random.randint(jax.random.fold_in(own_key, axis), (), 0, length) for axis, length in enumerate(result.shape)]
    main_axis = result.shape.index(max(result.shape))
    next_to = spot[:main_axis] + [(spot[main_axis] + 1) % result.shape[main_axis]] + spot[main_axis + 1:]
    return result.at[tuple(spot)].set(least).at[tuple(next_to)].set(high)


def steps_of(stream_key, extent, cuts, least, largest):
    def one(dim, parts):
        draws = jax.random.uniform(jax.random.fold_in(jax.random.fold_in(stream_key, 6), dim), (parts,), jnp.float32, least / len(cuts), largest / len(cuts))
        return jnp.repeat(jnp.exp(draws), extent[dim] // parts).reshape((-1,) + (1,) * (len(extent) - dim - 1))

    loudness = one(*cuts[0])
    for cut in cuts[1:]:
        loudness = loudness * one(*cut)
    return loudness


def gaussian(key, shape, scale, most, cuts=(), kind=jnp.bfloat16):
    gain = steps_of(key, shape, cuts, -0.22, 0.18) if cuts else 1.0
    result = jax.random.normal(key, shape, jnp.float32) * scale * gain
    return jnp.minimum(jnp.maximum(result, -most), most).astype(kind)


def setup_inputs(seed: int = 0) -> dict:
    key_of = jax.random.split(jax.random.key(seed), 7)
    return {
        "sample_fields": gaussian(key_of[0], (MEMBERS, 3, NX, NY), 0.2, 0.8, ((0, 16), (2, 8)), jnp.float32),
        "report_counts": draw_report_counts(jax.random.fold_in(key_of[6], 71), 0),
        "report_cells": with_ends(jax.random.randint(key_of[2], (NORTHWARD_PATCHES, EASTWARD_PATCHES, OBS_MAX), 0, BAND_HEIGHT_CELLS * PATCH_WIDTH_CELLS), jax.random.fold_in(key_of[2], 1), 0, (BAND_HEIGHT_CELLS * PATCH_WIDTH_CELLS) - 1).astype(jnp.int32),
        "report_values": gaussian(key_of[3], (NORTHWARD_PATCHES, EASTWARD_PATCHES, OBS_MAX), 0.3, 1.5, ((0, 8), (1, 16)), jnp.float32),
        "report_errors": jnp.clip(jnp.exp(math.log(0.2) - 1.609438 * jax.random.uniform(key_of[4], (NORTHWARD_PATCHES, EASTWARD_PATCHES, OBS_MAX), jnp.float32) ** steps_of(key_of[4], (NORTHWARD_PATCHES, EASTWARD_PATCHES, OBS_MAX), ((0, 8), (1, 16)), -0.2, 0.2)), 0.04, 0.2),
        "local_radius": with_ends(jax.random.randint(key_of[5], (NORTHWARD_PATCHES, EASTWARD_PATCHES), 1, 4), jax.random.fold_in(key_of[5], 1), 1, 3).astype(jnp.int32),
    }


COURANT = 0.125
GRAVITY = 1.0
ROTATION = 0.05
HIGHEST_PRECISION = lax.Precision.HIGHEST

def to_east(field):
    return field[..., 1:-1, 2:]

def to_west(field):
    return field[..., 1:-1, :-2]

def to_north(field):
    return field[..., 2:, 1:-1]

def to_south(field):
    return field[..., :-2, 1:-1]

def middle(field):
    return field[..., 1:-1, 1:-1]

def neighbour_mean(field):
    return 0.25 * (to_east(field) + to_west(field) + to_north(field) + to_south(field))

def advance_once(padded):
    height = padded[:, 0]
    flow_x = padded[:, 1]
    flow_y = padded[:, 2]
    column_depth = 1.0 + height
    flux_x = column_depth * flow_x
    flux_y = column_depth * flow_y
    centre_x = middle(flow_x)
    centre_y = middle(flow_y)
    new_height = neighbour_mean(height) - COURANT * (to_east(flux_x) - to_west(flux_x) + to_north(flux_y) - to_south(flux_y))
    new_flow_x = neighbour_mean(flow_x) - COURANT * (centre_x * (to_east(flow_x) - to_west(flow_x)) + centre_y * (to_north(flow_x) - to_south(flow_x)) + GRAVITY * (to_east(height) - to_west(height))) + ROTATION * centre_y
    new_flow_y = neighbour_mean(flow_y) - COURANT * (centre_x * (to_east(flow_y) - to_west(flow_y)) + centre_y * (to_north(flow_y) - to_south(flow_y)) + GRAVITY * (to_north(height) - to_south(height))) - ROTATION * centre_x
    return jnp.stack([new_height, new_flow_x, new_flow_y], axis=1)

def observe(region, locations, values, errors, live_count):
    observed = jnp.take(region, locations, axis=1)
    observed_mean = lax.optimization_barrier(jnp.mean(observed, axis=0))
    spread = observed - observed_mean[None, :]
    innovation = values - observed_mean
    slot_ids = jnp.arange(locations.shape[0])
    precision = jnp.where(slot_ids < live_count, 1.0 / errors, 0.0 * errors)
    row_pos = ((locations // PATCH_WIDTH_CELLS).astype(jnp.float32) + 0.5) / BAND_HEIGHT_CELLS - 0.5
    col_pos = ((locations % PATCH_WIDTH_CELLS).astype(jnp.float32) + 0.5) / PATCH_WIDTH_CELLS - 0.5
    row_pos = row_pos.astype(errors.dtype)
    col_pos = col_pos.astype(errors.dtype)
    return jnp.concatenate([spread, innovation[None], precision[None], row_pos[None], col_pos[None]], axis=0)

def analyse(region, neighbours, radius_blocks):
    sample_collection = region.shape[0]
    offsets = jnp.arange(3).astype(region.dtype) - 1.0
    anomalies = neighbours[:, :, :sample_collection, :]
    innovation = neighbours[:, :, sample_collection, :].reshape(-1)
    precision = neighbours[:, :, sample_collection + 1, :]
    row_pos = neighbours[:, :, sample_collection + 2, :] + offsets[:, None, None]
    col_pos = neighbours[:, :, sample_collection + 3, :] + offsets[None, :, None]
    radius_float = radius_blocks.astype(region.dtype)
    tapering = jnp.exp(-0.5 * (row_pos * row_pos + col_pos * col_pos) / (radius_float * radius_float))
    weights = (tapering * precision).reshape(-1)
    spread = jnp.transpose(anomalies, (2, 0, 1, 3)).reshape(sample_collection, -1)
    weighted = spread * weights[None, :]
    ensemble_scale = sample_collection - 1.0
    identity = jnp.eye(sample_collection, dtype=region.dtype)
    gram_matrix = jnp.dot(weighted, spread.T, precision=HIGHEST_PRECISION)
    normal = identity + gram_matrix / ensemble_scale
    pull_vector = jnp.dot(weighted, innovation, precision=HIGHEST_PRECISION)
    frob_norm = jnp.sqrt(jnp.sum(normal * normal))
    iterate = normal / frob_norm
    inverse_root = identity
    for newton_turn in range(TURNS):
        factor = 1.5 * identity - 0.5 * jnp.dot(inverse_root, iterate, precision=HIGHEST_PRECISION)
        iterate = jnp.dot(iterate, factor, precision=HIGHEST_PRECISION)
        inverse_root = jnp.dot(factor, inverse_root, precision=HIGHEST_PRECISION)
    root_inverse = inverse_root / jnp.sqrt(frob_norm)
    full_inverse = jnp.dot(inverse_root, inverse_root, precision=HIGHEST_PRECISION) / frob_norm
    mean_weights = jnp.dot(full_inverse, pull_vector, precision=HIGHEST_PRECISION) / ensemble_scale
    transform = root_inverse + mean_weights[:, None]
    centre = lax.optimization_barrier(jnp.mean(region, axis=0))
    deviations = region - centre[None, :]
    return centre[None, :] + jnp.dot(transform.T, deviations, precision=HIGHEST_PRECISION)

def single_prediction(sample_conditions):
    for repeat in range(STEPS):
        padded = jnp.pad(sample_conditions[None], ((0, 0), (0, 0), (1, 1), (1, 1)), mode='wrap')
        sample_conditions = advance_once(padded)[0]
    return sample_conditions

def reference(sample_fields, report_counts, report_cells, report_values, report_errors, local_radius):
    sample_collection = sample_fields.shape[0]
    predicted_samples = lax.map(single_prediction, sample_fields)
    patch_nearby = predicted_samples.reshape(sample_collection, 3, NORTHWARD_PATCHES, BAND_HEIGHT_CELLS, EASTWARD_PATCHES, PATCH_WIDTH_CELLS)
    patch_nearby = jnp.transpose(patch_nearby, (2, 4, 0, 1, 3, 5)).reshape(NORTHWARD_PATCHES, EASTWARD_PATCHES, sample_collection, 3 * BAND_HEIGHT_CELLS * PATCH_WIDTH_CELLS)
    packed = jax.vmap(jax.vmap(observe))(patch_nearby, report_cells, report_values, report_errors, report_counts)
    stacked_rows = []
    for first in range(3):
        stacked_cols = []
        for second in range(3):
            stacked_cols.append(jnp.roll(packed, (1 - first, 1 - second), axis=(0, 1)))
        stacked_rows.append(jnp.stack(stacked_cols, axis=2))
    neighbours = jnp.stack(stacked_rows, axis=2)
    updated = jax.vmap(jax.vmap(analyse))(patch_nearby, neighbours, local_radius)
    updated = updated.reshape(NORTHWARD_PATCHES, EASTWARD_PATCHES, sample_collection, 3, BAND_HEIGHT_CELLS, PATCH_WIDTH_CELLS)
    updated = jnp.transpose(updated, (2, 3, 0, 4, 1, 5))
    return updated.reshape(sample_collection, 3, NORTHWARD_PATCHES * BAND_HEIGHT_CELLS, EASTWARD_PATCHES * PATCH_WIDTH_CELLS)
```

```python
import jax
import jax.numpy as jnp
from jax import lax
from jax.experimental import pallas as pl
from jax.experimental.pallas import tpu as pltpu
from jax.sharding import PartitionSpec as P

STEPS = 12
TURNS = 20
MEMBERS = 64
OWN = 4
STRIPS = 8
OWNERS = 16
ROWS = 16
COLS = 128
BLOCK = 256
OBS = 256
EDGE = 16
GUARD = 8
FIRST = GUARD + EDGE
SPAN = BLOCK + 2 * EDGE + 2 * GUARD
UNROLL = 6
MESH = pl.DeviceIdType.MESH
F32 = jnp.float32
BF16 = jnp.bfloat16


def block_of(strip):
    z, xh = strip // 2, strip % 2
    return z + xh * (7 - 2 * z)


def strip_of(block):
    return 2 * block + (block // 4) * (15 - 4 * block)


def region_of(i, strip):
    y, c, z = (i // 2) % 4, i % 2, strip // 2
    return 2 * ((y + z) % 4) + (c + y) % 2, i // 8


def owner_of(a, b):
    strip = strip_of(b // 2)
    y = (a // 2 + 4 - strip // 2) % 4
    return (b % 2) * 8 + y * 2 + (a + y) % 2, strip


def remote(src, dst, send, recv, where):
    return pltpu.make_async_remote_copy(
        src_ref=src, dst_ref=dst, send_sem=send, recv_sem=recv, device_id=where, device_id_type=MESH
    )


def halves(value):
    high = value.astype(BF16)
    return high, (value - high.astype(F32)).astype(BF16)


def thirds(value):
    high = value.astype(BF16)
    rest = value - high.astype(F32)
    mid = rest.astype(BF16)
    return high, mid, (rest - mid.astype(F32)).astype(BF16)


def dot(a, b):
    return jnp.dot(a, b, preferred_element_type=F32)


def matmul(a, b):
    ah, al = halves(a)
    bh, bl = halves(b)
    return dot(ah, bh) + (dot(ah, bl) + dot(al, bh))


def turn_north(value):
    return pltpu.roll(value, COLS - 1, 1)


def turn_south(value):
    return pltpu.roll(value, 1, 1)


def step_rows(src, dst, at):
    rows = pl.ds(at, 8)
    east, west = pl.ds(at + 1, 8), pl.ds(at - 1, 8)
    h, p, q = src[0, rows], src[1, rows], src[2, rows]
    he, pe, qe = src[0, east], src[1, east], src[2, east]
    hw, pw, qw = src[0, west], src[1, west], src[2, west]
    a, a2, b, b2 = 0.25 - p, 0.25 + p, 0.25 - q, 0.25 + q
    pn, ps = turn_north(p), turn_south(p)
    qn, qs = turn_north(q), turn_south(q)
    hn, hs = turn_north(h), turn_south(h)
    flow = (pe - pw) + (qn - qs)
    dst[0, rows] = (
        (he * (0.25 - pe) + hw * (0.25 + pw)) + (turn_north(h * b) + turn_south(h * b2))
    ) - (1.0 / 64.0) * flow
    dst[1, rows] = ((a * pe + a2 * pw) + (b * pn + b2 * ps)) + (0.05 * q - (he - hw))
    dst[2, rows] = ((a * qe + a2 * qw) + (b * qn + b2 * qs)) - (0.05 * p + (hn - hs))


def kernel(
    x, cells, values, errors, count, radius, out,
    landed, work, edge, halo, staged, region, mixed, packed, own, reach, near, onehot, tall_h, tall_l, roots, mix_h, mix_l, gram,
    grams,
    send1, recv1, send_edge, recv_edge, send2, recv2, send_obs, recv_obs, recv_reach,
    send_gram, recv_gram, send3, recv3,
):
    i = lax.axis_index("member")
    s = lax.axis_index("strip")
    t = block_of(s)
    a, b0 = region_of(i, s)
    b = 2 * t + b0

    for j in range(OWN):
        for d in range(1, STRIPS):
            to = lax.rem(s + d, STRIPS)
            remote(
                x.at[j, :, :, pl.ds(pl.multiple_of(block_of(to) * BLOCK, BLOCK), BLOCK)],
                landed.at[j, :, pl.ds(pl.multiple_of(s * ROWS, ROWS), ROWS)],
                send1.at[j], recv1.at[j], (i, to),
            ).start()
        pltpu.make_async_copy(
            x.at[j, :, :, pl.ds(pl.multiple_of(t * BLOCK, BLOCK), BLOCK)],
            landed.at[j, :, pl.ds(pl.multiple_of(s * ROWS, ROWS), ROWS)],
            recv1.at[j],
        ).start()

    slots = lax.broadcasted_iota(jnp.int32, (1, OBS), 1)
    packed[0:1] = cells[...].astype(F32)
    packed[1:2] = values[...]
    packed[2:3] = jnp.where(slots < count[0, 0], 1.0 / errors[...], 0.0)
    reach[...] = jnp.full((8, COLS), radius[0, 0], jnp.int32).astype(F32)
    to_i, to_s = owner_of(s, i)
    mine = (to_i == i) & (to_s == s)

    @pl.when(mine)
    def _():
        pltpu.make_async_copy(packed, own, recv_obs).start()

    @pl.when(jnp.logical_not(mine))
    def _():
        remote(packed, own, send_obs.at[9], recv_obs, (to_i, to_s)).start()

    def each_near(act_local, act_remote):
        for k in range(9):
            n_i, n_s = owner_of((s + k // 3 + 7) % 8, (i + k % 3 + 15) % 16)
            self = (n_i == i) & (n_s == s)
            if act_local is not None:
                pl.when(self)(lambda k=k: act_local(k))
            pl.when(jnp.logical_not(self))(lambda k=k, n_i=n_i, n_s=n_s: act_remote(k, n_i, n_s))

    each_near(
        lambda k: pltpu.make_async_copy(reach, near.at[k], recv_reach).start(),
        lambda k, n_i, n_s: remote(
            reach, near.at[k], send_obs.at[k], recv_reach, (n_i, n_s)
        ).start(),
    )

    left = (i, strip_of((t + 7) % 8))
    right = (i, strip_of((t + 1) % 8))
    for c in range(2):
        for g in range(2):
            for f in range(3):
                work[c, g, f, 0:GUARD] = jnp.zeros((GUARD, COLS), F32)
                work[c, g, f, SPAN - GUARD : SPAN] = jnp.zeros((GUARD, COLS), F32)

    def edge_copies(j):
        return (
            remote(
                edge.at[j, 0], halo.at[j, 1], send_edge.at[j, 0], recv_edge.at[j, 1], left
            ),
            remote(
                edge.at[j, 1], halo.at[j, 0], send_edge.at[j, 1], recv_edge.at[j, 0], right
            ),
        )

    def arrive(j):
        pltpu.make_async_copy(landed.at[j], landed.at[j], recv1.at[j]).wait()
        buf = work.at[j % 2, 0]
        for f in range(3):
            scale = 1.0 / 64.0 if f == 0 else 0.125
            for c in range(2):
                turned = landed[j, f, :, c * COLS : (c + 1) * COLS].T * scale
                buf[f, FIRST + c * COLS : FIRST + (c + 1) * COLS] = turned
                if c == 0:
                    edge[j, 0, f] = turned[:EDGE]
                else:
                    edge[j, 1, f] = turned[COLS - EDGE :]
        for copy in edge_copies(j):
            copy.start()

    def forecast(j):
        for copy in edge_copies(j):
            copy.wait_recv()
        ping, pong = work.at[j % 2, 0], work.at[j % 2, 1]
        for f in range(3):
            ping[f, GUARD:FIRST] = halo[j, 0, f]
            ping[f, FIRST + BLOCK : FIRST + BLOCK + EDGE] = halo[j, 1, f]

        def sweep(src, dst):
            def chunk(n, _):
                at = pl.multiple_of(n * (8 * UNROLL), 8) + GUARD
                for u in range(UNROLL):
                    step_rows(src, dst, at + 8 * u)
                return 0

            lax.fori_loop(0, (SPAN - 2 * GUARD) // (8 * UNROLL), chunk, 0)

        def two_steps(n, _):
            sweep(ping, pong)
            sweep(pong, ping)
            return 0

        lax.fori_loop(0, STEPS // 2, two_steps, 0)
        for f in range(3):
            scale = 64.0 if f == 0 else 8.0
            for c in range(2):
                block = ping[f, FIRST + c * COLS : FIRST + (c + 1) * COLS]
                staged[j, f, :, c * COLS : (c + 1) * COLS] = block.T * scale
        for d in range(OWNERS):
            to = lax.rem(i + d, OWNERS)
            to_a, to_b0 = region_of(to, s)
            src = staged.at[
                j, :, pl.ds(pl.multiple_of(to_a * ROWS, ROWS), ROWS),
                pl.ds(pl.multiple_of(to_b0 * COLS, COLS), COLS),
            ]
            dst = region.at[:, :, OWN * i + j]
            if d == 0:
                pltpu.make_async_copy(src, dst, recv2).start()
            else:
                remote(src, dst, send2, recv2, (to, s)).start()

    arrive(0)
    arrive(1)
    pltpu.make_async_copy(own, own, recv_obs).wait()
    place = own[0:1]

    def mark(n, _):
        at = pl.multiple_of(n * COLS, COLS)
        cell = lax.broadcasted_iota(jnp.int32, (COLS, OBS), 0) + at
        onehot[pl.ds(at, COLS)] = jnp.where(cell.astype(F32) == place, 1.0, 0.0).astype(BF16)
        return 0

    lax.fori_loop(0, ROWS, mark, 0)
    forecast(0)
    arrive(2)
    forecast(1)
    arrive(3)
    forecast(2)
    forecast(3)

    pltpu.make_async_copy(region, region, recv2).wait()

    def look(n, height):
        pair = jnp.concatenate([region[0, 2 * n], region[0, 2 * n + 1]], axis=1)
        marks = onehot[pl.ds(pl.multiple_of(n * OBS, OBS), OBS)]
        high, mid, low = thirds(pair)
        return height + (dot(high, marks) + (dot(mid, marks) + dot(low, marks)))

    height = lax.fori_loop(0, ROWS // 2, look, jnp.zeros((MEMBERS, OBS), F32))
    mean = jnp.mean(height, axis=0, keepdims=True)
    spread = height - mean
    innovation = own[1:2] - mean
    precision = own[2:3]
    line = jnp.floor(place * (1.0 / COLS))
    row_pos = (line + 0.5) * (1.0 / ROWS) - 0.5
    col_pos = (place - line * COLS + 0.5) * (1.0 / COLS) - 0.5
    wide = jnp.concatenate(
        [spread, innovation, jnp.zeros((COLS - MEMBERS - 1, OBS), F32)], axis=0
    )
    tall = jnp.concatenate([wide[:, :COLS].T, wide[:, COLS:].T], axis=0)
    columns_h, columns_l = halves(tall)
    tall_h[...], tall_l[...] = columns_h, columns_l
    pltpu.make_async_copy(near, near, recv_reach).wait()

    def product(k, _):
        r = row_pos + (k // 3 - 1).astype(F32)
        c = col_pos + (k % 3 - 1).astype(F32)
        radius_k = near[k, 0:1, 0:1]
        taper = jnp.exp(-0.5 * (r * r + c * c) / (radius_k * radius_k))
        wh, wl = halves(spread * (taper * precision))
        gram[k] = dot(wh, tall_h[...]) + (dot(wh, tall_l[...]) + dot(wl, tall_h[...]))
        return 0

    lax.fori_loop(0, 9, product, 0)

    def gram_copy(k):
        to = owner_of((a + 9 - k // 3) % 8, (b + 17 - k % 3) % 16)
        return remote(gram.at[k], grams.at[k], send_gram.at[k], recv_gram.at[k], to)

    for k in range(9):
        if k != 4:
            gram_copy(k).start()
    total = gram[4]
    for k in range(9):
        if k != 4:
            gram_copy(k).wait_recv()
            total = total + grams[k]

    scale = 1.0 / (MEMBERS - 1.0)
    eye = (
        lax.broadcasted_iota(jnp.int32, (MEMBERS, MEMBERS), 0)
        == lax.broadcasted_iota(jnp.int32, (MEMBERS, MEMBERS), 1)
    ).astype(F32)
    normal = eye + total[:, :MEMBERS] * scale
    frob2 = jnp.sum(jnp.sum(normal * normal, axis=1, keepdims=True), axis=0, keepdims=True)
    frob = jnp.sqrt(frob2)

    roots[0], roots[1] = normal / frob, eye

    def turn(_, carry):
        u, z = roots[0], roots[1]
        factor = 1.5 * eye - 0.5 * matmul(z, u)
        roots[0], roots[1] = matmul(u, factor), matmul(factor, z)
        return carry

    lax.fori_loop(0, TURNS, turn, 0)
    inverse = roots[1]
    pull = matmul(inverse, matmul(inverse, total)) / frob
    lane = lax.broadcasted_iota(jnp.int32, (MEMBERS, COLS), 1)
    mean_weights = jnp.sum(jnp.where(lane == MEMBERS, pull, 0.0), axis=1, keepdims=True) * scale
    transform = inverse / jnp.sqrt(frob) + mean_weights
    padded = jnp.concatenate(
        [
            jnp.concatenate([transform, jnp.zeros((MEMBERS, MEMBERS), F32)], axis=1),
            jnp.zeros((MEMBERS, COLS), F32),
        ],
        axis=0,
    )
    weights_h, weights_l = halves(padded.T[:MEMBERS])
    mix_h[...], mix_l[...] = weights_h, weights_l

    here = a == s
    columns = pl.ds(pl.multiple_of(b * COLS, COLS), COLS)
    for f in range(3):

        def rows_of(n, _):
            pair = jnp.concatenate([region[f, 2 * n], region[f, 2 * n + 1]], axis=1)
            centre = jnp.mean(pair, axis=0, keepdims=True)
            dev_h, dev_l = halves(pair - centre)
            result = centre + (
                dot(mix_h[:, :MEMBERS], dev_h)
                + (dot(mix_h[:, :MEMBERS], dev_l) + dot(mix_l[:, :MEMBERS], dev_h))
            )
            mixed[f, 2 * n] = result[:, :COLS]
            mixed[f, 2 * n + 1] = result[:, COLS:]
            return 0

        lax.fori_loop(0, ROWS // 2, rows_of, 0)
        for d in range(OWNERS):
            to = lax.rem(i + d, OWNERS)
            for j in range(OWN):
                src = mixed.at[f, :, OWN * to + j]
                dst = out.at[j, f, :, columns]
                if d == 0:
                    pl.when(here)(
                        lambda src=src, dst=dst: pltpu.make_async_copy(
                            src, dst, recv3
                        ).start()
                    )
                    pl.when(jnp.logical_not(here))(
                        lambda src=src, dst=dst: remote(
                            src, dst, send3.at[1], recv3, (i, a)
                        ).start()
                    )
                else:
                    remote(src, dst, send3.at[0], recv3, (to, a)).start()

    for j in range(OWN):
        rest = landed.at[j, :, pl.ds(0, ROWS * (STRIPS - 1))]
        remote(rest, rest, send1.at[j], recv1.at[j], (i, s)).wait_send()
        for copy in edge_copies(j):
            copy.wait_send()
    pl.when(jnp.logical_not(mine))(
        lambda: remote(packed, own, send_obs.at[9], recv_obs, (i, s)).wait_send()
    )
    each_near(
        None,
        lambda k, n_i, n_s: remote(
            reach, near.at[k], send_obs.at[k], recv_reach, (n_i, n_s)
        ).wait_send(),
    )
    rest = region.at[:, :, pl.ds(0, OWN * (OWNERS - 1))]
    remote(rest, rest, send2, recv2, (i, s)).wait_send()
    for k in range(9):
        if k != 4:
            gram_copy(k).wait_send()
    remote(rest, rest, send3.at[0], recv3, (i, s)).wait_send()
    few = region.at[:, :, pl.ds(0, OWN)]
    pl.when(jnp.logical_not(here))(
        lambda: remote(few, few, send3.at[1], recv3, (i, s)).wait_send()
    )
    remote(out, out, send3.at[0], recv3, (i, s)).wait_recv()


def on_device(fields, counts, cells, values, errors, radius):
    vmem = pl.BlockSpec(memory_space=pltpu.VMEM)
    smem = pl.BlockSpec(memory_space=pltpu.SMEM)
    hbm = pl.BlockSpec(memory_space=pl.ANY)
    dma = pltpu.SemaphoreType.DMA
    return pl.pallas_call(
        kernel,
        out_shape=jax.ShapeDtypeStruct(fields.shape, F32),
        in_specs=[hbm, vmem, vmem, vmem, smem, smem],
        out_specs=hbm,
        scratch_shapes=[
            pltpu.VMEM((OWN, 3, STRIPS * ROWS, BLOCK), F32),
            pltpu.VMEM((2, 2, 3, SPAN, COLS), F32),
            pltpu.VMEM((OWN, 2, 3, EDGE, COLS), F32),
            pltpu.VMEM((OWN, 2, 3, EDGE, COLS), F32),
            pltpu.VMEM((OWN, 3, STRIPS * ROWS, BLOCK), F32),
            pltpu.VMEM((3, ROWS, MEMBERS, COLS), F32),
            pltpu.VMEM((3, ROWS, MEMBERS, COLS), F32),
            pltpu.VMEM((8, OBS), F32),
            pltpu.VMEM((8, OBS), F32),
            pltpu.VMEM((8, COLS), F32),
            pltpu.VMEM((9, 8, COLS), F32),
            pltpu.VMEM((ROWS * COLS, OBS), BF16),
            pltpu.VMEM((OBS, COLS), BF16),
            pltpu.VMEM((OBS, COLS), BF16),
            pltpu.VMEM((2, MEMBERS, MEMBERS), F32),
            pltpu.VMEM((MEMBERS, COLS), BF16),
            pltpu.VMEM((MEMBERS, COLS), BF16),
            pltpu.VMEM((9, MEMBERS, COLS), F32),
            pltpu.VMEM((9, MEMBERS, COLS), F32),
            dma((OWN,)), dma((OWN,)), dma((OWN, 2)), dma((OWN, 2)), dma, dma, dma((10,)), dma, dma,
            dma((9,)), dma((9,)), dma((2,)), dma,
        ],
        compiler_params=pltpu.CompilerParams(
            has_side_effects=True, vmem_limit_bytes=40 * 1024 * 1024
        ),
        name="forecast_and_analysis",
    )(
        fields, cells.reshape(1, OBS), values.reshape(1, OBS), errors.reshape(1, OBS),
        counts, radius,
    )


def solution(mesh):
    in_specs = (
        P("member", None, "strip", None),
        P("strip", "member"),
        P("strip", "member", None),
        P("strip", "member", None),
        P("strip", "member", None),
        P("strip", "member"),
    )
    return jax.shard_map(
        on_device, mesh=mesh, in_specs=in_specs, out_specs=P("member", None, "strip", None),
        check_vma=False,
    )
```

```python
import jax
import jax.numpy as jnp
from jax import lax
from jax.experimental import pallas as pl
from jax.experimental.pallas import tpu as pltpu
from jax.sharding import PartitionSpec as P

STEPS = 12
TURNS = 20
MEMBERS = 64
OWN = 4
STRIPS = 8
OWNERS = 16
ROWS = 16
COLS = 128
BLOCK = 256
OBS = 256
EDGE = 16
GUARD = 8
FIRST = GUARD + EDGE
SPAN = BLOCK + 2 * EDGE + 2 * GUARD
MESH = pl.DeviceIdType.MESH
F32 = jnp.float32
BF16 = jnp.bfloat16


def block_of(strip):
    z, xh = strip // 2, strip % 2
    return z + xh * (7 - 2 * z)


def strip_of(block):
    return 2 * block + (block // 4) * (15 - 4 * block)


def region_of(i, strip):
    y, c, z = (i // 2) % 4, i % 2, strip // 2
    return 2 * ((y + z) % 4) + (c + y) % 2, i // 8


def owner_of(a, b):
    strip = strip_of(b // 2)
    y = (a // 2 + 4 - strip // 2) % 4
    return (b % 2) * 8 + y * 2 + (a + y) % 2, strip


def remote(src, dst, send, recv, where):
    return pltpu.make_async_remote_copy(
        src_ref=src, dst_ref=dst, send_sem=send, recv_sem=recv, device_id=where, device_id_type=MESH
    )


def halves(value):
    high = value.astype(BF16)
    return high, (value - high.astype(F32)).astype(BF16)


def thirds(value):
    high = value.astype(BF16)
    rest = value - high.astype(F32)
    mid = rest.astype(BF16)
    return high, mid, (rest - mid.astype(F32)).astype(BF16)


def dot(a, b):
    return jnp.dot(a, b, preferred_element_type=F32)


def matmul(a, b):
    ah, al = halves(a)
    bh, bl = halves(b)
    return dot(ah, bh) + (dot(ah, bl) + dot(al, bh))


def turn_north(value):
    return pltpu.roll(value, COLS - 1, 1)


def turn_south(value):
    return pltpu.roll(value, 1, 1)


def step_rows(src, dst, at):
    rows = pl.ds(at, 8)
    east, west = pl.ds(at + 1, 8), pl.ds(at - 1, 8)
    h, p, q = src[0, rows], src[1, rows], src[2, rows]
    he, pe, qe = src[0, east], src[1, east], src[2, east]
    hw, pw, qw = src[0, west], src[1, west], src[2, west]
    a, a2, b, b2 = 0.25 - p, 0.25 + p, 0.25 - q, 0.25 + q
    pn, ps = turn_north(p), turn_south(p)
    qn, qs = turn_north(q), turn_south(q)
    hn, hs = turn_north(h), turn_south(h)
    flow = (pe - pw) + (qn - qs)
    dst[0, rows] = (
        (he * (0.25 - pe) + hw * (0.25 + pw)) + (hn * (0.25 - qn) + hs * (0.25 + qs))
    ) - (1.0 / 64.0) * flow
    dst[1, rows] = ((a * pe + a2 * pw) + (b * pn + b2 * ps)) + (0.05 * q - (he - hw))
    dst[2, rows] = ((a * qe + a2 * qw) + (b * qn + b2 * qs)) - (0.05 * p + (hn - hs))


def kernel(
    x, cells, values, errors, count, radius, out,
    raw_cells, raw, raw_scalars, raw_radius, landed, work, edge, halo, staged, region, mixed, packed, own, reach, near, onehot, tall_h, tall_l, roots, mix_h, mix_l, gram,
    grams,
    load_sem, send1, recv1, send_edge, recv_edge, send2, recv2, send_obs, recv_obs, recv_reach,
    send_gram, recv_gram, send3, recv3,
):
    i = lax.axis_index("member")
    s = lax.axis_index("strip")
    t = block_of(s)
    a, b0 = region_of(i, s)
    b = 2 * t + b0

    def neighbour(k):
        return owner_of((a + 7 + k // 3) % 8, (b + 15 + k % 3) % 16)

    to_i, to_s = owner_of(s, i)
    mine = (to_i == i) & (to_s == s)
    here = a == s
    loads = [
        pltpu.make_async_copy(cells, raw_cells, load_sem.at[0]),
        pltpu.make_async_copy(values, raw.at[0:1], load_sem.at[1]),
        pltpu.make_async_copy(errors, raw.at[1:2], load_sem.at[2]),
        pltpu.make_async_copy(count, raw_scalars, load_sem.at[3]),
        pltpu.make_async_copy(radius, raw_radius, load_sem.at[4]),
    ]
    for copy in loads:
        copy.start()

    barrier = pltpu.get_barrier_semaphore()

    def greet(where):
        pl.semaphore_signal(barrier, inc=1, device_id=where, device_id_type=MESH)

    for k in range(9):
        if k != 4:
            greet(neighbour(k))
    for n in range(OWNERS):
        sender = owner_of(s, n)
        pl.when((sender[0] != i) | (sender[1] != s))(lambda sender=sender: greet(sender))
    pl.when((b != i) | (a != s))(lambda: greet((b, a)))
    for d in range(1, OWNERS):
        greet((lax.rem(i + d, OWNERS), s))
    for d in range(1, STRIPS):
        greet((i, lax.rem(s + d, STRIPS)))
    pl.semaphore_wait(
        barrier,
        8 + OWNERS + 1 + (OWNERS - 1) + (STRIPS - 1)
        - mine.astype(jnp.int32) - here.astype(jnp.int32),
    )

    for j in range(OWN):
        for d in range(1, STRIPS):
            to = lax.rem(s + d, STRIPS)
            remote(
                x.at[j, :, :, pl.ds(pl.multiple_of(block_of(to) * BLOCK, BLOCK), BLOCK)],
                landed.at[j, :, pl.ds(pl.multiple_of(s * ROWS, ROWS), ROWS)],
                send1.at[j], recv1.at[j], (i, to),
            ).start()
        pltpu.make_async_copy(
            x.at[j, :, :, pl.ds(pl.multiple_of(t * BLOCK, BLOCK), BLOCK)],
            landed.at[j, :, pl.ds(pl.multiple_of(s * ROWS, ROWS), ROWS)],
            recv1.at[j],
        ).start()

    for copy in loads:
        copy.wait()
    slots = lax.broadcasted_iota(jnp.int32, (1, OBS), 1)
    packed[0:1] = raw_cells[...].astype(F32)
    packed[1:2] = raw[0:1]
    packed[2:3] = jnp.where(slots < raw_scalars[0:1, 0:1], 1.0 / raw[1:2], 0.0)
    packed[3:4] = jnp.broadcast_to(raw_radius[0:1, 0:1].astype(F32), (1, OBS))

    @pl.when(mine)
    def _():
        pltpu.make_async_copy(packed, own, recv_obs).start()

    @pl.when(jnp.logical_not(mine))
    def _():
        remote(packed, own, send_obs.at[9], recv_obs, (to_i, to_s)).start()

    left = (i, strip_of((t + 7) % 8))
    right = (i, strip_of((t + 1) % 8))
    for c in range(2):
        for g in range(2):
            for f in range(3):
                work[c, g, f, 0:GUARD] = jnp.zeros((GUARD, COLS), F32)
                work[c, g, f, SPAN - GUARD : SPAN] = jnp.zeros((GUARD, COLS), F32)

    def edge_copies(j):
        return (
            remote(
                edge.at[j, 0], halo.at[j, 1], send_edge.at[j, 0], recv_edge.at[j, 1], left
            ),
            remote(
                edge.at[j, 1], halo.at[j, 0], send_edge.at[j, 1], recv_edge.at[j, 0], right
            ),
        )

    def arrive(j):
        pltpu.make_async_copy(landed.at[j], landed.at[j], recv1.at[j]).wait()
        buf = work.at[j % 2, 0]
        for f in range(3):
            scale = 1.0 / 64.0 if f == 0 else 0.125
            for c in range(2):
                turned = landed[j, f, :, c * COLS : (c + 1) * COLS].T * scale
                buf[f, FIRST + c * COLS : FIRST + (c + 1) * COLS] = turned
                if c == 0:
                    edge[j, 0, f] = turned[:EDGE]
                else:
                    edge[j, 1, f] = turned[COLS - EDGE :]
        for copy in edge_copies(j):
            copy.start()

    def forecast(j):
        for copy in edge_copies(j):
            copy.wait_recv()
        ping, pong = work.at[j % 2, 0], work.at[j % 2, 1]
        for f in range(3):
            ping[f, GUARD:FIRST] = halo[j, 0, f]
            ping[f, FIRST + BLOCK : FIRST + BLOCK + EDGE] = halo[j, 1, f]

        def sweep(src, dst):
            for n in range((SPAN - 2 * GUARD) // 8):
                step_rows(src, dst, GUARD + 8 * n)

        def two_steps(n, _):
            sweep(ping, pong)
            sweep(pong, ping)
            return 0

        lax.fori_loop(0, STEPS // 2, two_steps, 0)
        for f in range(3):
            scale = 64.0 if f == 0 else 8.0
            for c in range(2):
                block = ping[f, FIRST + c * COLS : FIRST + (c + 1) * COLS]
                staged[j, f, :, c * COLS : (c + 1) * COLS] = block.T * scale
        for d in range(OWNERS):
            to = lax.rem(i + d, OWNERS)
            to_a, to_b0 = region_of(to, s)
            src = staged.at[
                j, :, pl.ds(pl.multiple_of(to_a * ROWS, ROWS), ROWS),
                pl.ds(pl.multiple_of(to_b0 * COLS, COLS), COLS),
            ]
            dst = region.at[:, :, OWN * i + j]
            if d == 0:
                pltpu.make_async_copy(src, dst, recv2).start()
            else:
                remote(src, dst, send2, recv2, (to, s)).start()

    def reach_copy(k):
        return remote(
            reach, near.at[k], send_obs.at[k], recv_reach.at[k], neighbour(k)
        )

    arrive(0)
    arrive(1)
    pltpu.make_async_copy(own, own, recv_obs).wait()
    reach[...] = jnp.broadcast_to(own[3:4, :COLS], (8, COLS))
    for k in range(9):
        if k != 4:
            reach_copy(k).start()
    place = own[0:1]

    def mark(n, _):
        at = pl.multiple_of(n * COLS, COLS)
        cell = lax.broadcasted_iota(jnp.int32, (COLS, OBS), 0) + at
        onehot[pl.ds(at, COLS)] = jnp.where(cell.astype(F32) == place, 1.0, 0.0).astype(BF16)
        return 0

    lax.fori_loop(0, ROWS, mark, 0)
    forecast(0)
    arrive(2)
    forecast(1)
    arrive(3)
    forecast(2)
    forecast(3)

    pltpu.make_async_copy(region, region, recv2).wait()

    def look(n, height):
        pair = jnp.concatenate([region[0, 2 * n], region[0, 2 * n + 1]], axis=1)
        marks = onehot[pl.ds(pl.multiple_of(n * OBS, OBS), OBS)]
        high, mid, low = thirds(pair)
        return height + (dot(high, marks) + (dot(mid, marks) + dot(low, marks)))

    height = lax.fori_loop(0, ROWS // 2, look, jnp.zeros((MEMBERS, OBS), F32))
    mean = jnp.mean(height, axis=0, keepdims=True)
    spread = height - mean
    innovation = own[1:2] - mean
    precision = own[2:3]
    line = jnp.floor(place * (1.0 / COLS))
    row_pos = (line + 0.5) * (1.0 / ROWS) - 0.5
    col_pos = (place - line * COLS + 0.5) * (1.0 / COLS) - 0.5
    wide = jnp.concatenate(
        [spread, innovation, jnp.zeros((COLS - MEMBERS - 1, OBS), F32)], axis=0
    )
    tall = jnp.concatenate([wide[:, :COLS].T, wide[:, COLS:].T], axis=0)
    columns_h, columns_l = halves(tall)
    tall_h[...], tall_l[...] = columns_h, columns_l
    for k in range(9):
        if k != 4:
            reach_copy(k).wait_recv()
    near[4] = reach[...]

    def product(k, _):
        r = row_pos + (k // 3 - 1).astype(F32)
        c = col_pos + (k % 3 - 1).astype(F32)
        radius_k = near[k, 0:1, 0:1]
        taper = jnp.exp(-0.5 * (r * r + c * c) / (radius_k * radius_k))
        wh, wl = halves(spread * (taper * precision))
        gram[k] = dot(wh, tall_h[...]) + (dot(wh, tall_l[...]) + dot(wl, tall_h[...]))
        return 0

    lax.fori_loop(0, 9, product, 0)

    def gram_copy(k):
        return remote(
            gram.at[k], grams.at[k], send_gram.at[k], recv_gram.at[k], neighbour(8 - k)
        )

    for k in range(9):
        if k != 4:
            gram_copy(k).start()
    total = gram[4]
    for k in range(9):
        if k != 4:
            gram_copy(k).wait_recv()
            total = total + grams[k]

    scale = 1.0 / (MEMBERS - 1.0)
    eye = (
        lax.broadcasted_iota(jnp.int32, (MEMBERS, MEMBERS), 0)
        == lax.broadcasted_iota(jnp.int32, (MEMBERS, MEMBERS), 1)
    ).astype(F32)
    normal = eye + total[:, :MEMBERS] * scale
    frob2 = jnp.sum(jnp.sum(normal * normal, axis=1, keepdims=True), axis=0, keepdims=True)
    frob = jnp.sqrt(frob2)

    roots[0], roots[1] = normal / frob, eye

    def turn(_, carry):
        u, z = roots[0], roots[1]
        factor = 1.5 * eye - 0.5 * matmul(z, u)
        roots[0], roots[1] = matmul(u, factor), matmul(factor, z)
        return carry

    lax.fori_loop(0, TURNS, turn, 0)
    inverse = roots[1]
    pull = matmul(inverse, matmul(inverse, total)) / frob
    lane = lax.broadcasted_iota(jnp.int32, (MEMBERS, COLS), 1)
    mean_weights = jnp.sum(jnp.where(lane == MEMBERS, pull, 0.0), axis=1, keepdims=True) * scale
    transform = inverse / jnp.sqrt(frob) + mean_weights
    padded = jnp.concatenate(
        [
            jnp.concatenate([transform, jnp.zeros((MEMBERS, MEMBERS), F32)], axis=1),
            jnp.zeros((MEMBERS, COLS), F32),
        ],
        axis=0,
    )
    weights_h, weights_l = halves(padded.T[:MEMBERS])
    mix_h[...], mix_l[...] = weights_h, weights_l

    columns = pl.ds(pl.multiple_of(b * COLS, COLS), COLS)
    for f in range(3):

        def rows_of(n, _):
            pair = jnp.concatenate([region[f, 2 * n], region[f, 2 * n + 1]], axis=1)
            centre = jnp.mean(pair, axis=0, keepdims=True)
            dev_h, dev_l = halves(pair - centre)
            result = centre + (
                dot(mix_h[:, :MEMBERS], dev_h)
                + (dot(mix_h[:, :MEMBERS], dev_l) + dot(mix_l[:, :MEMBERS], dev_h))
            )
            mixed[f, 2 * n] = result[:, :COLS]
            mixed[f, 2 * n + 1] = result[:, COLS:]
            return 0

        lax.fori_loop(0, ROWS // 2, rows_of, 0)
        for d in range(OWNERS):
            to = lax.rem(i + d, OWNERS)
            for j in range(OWN):
                src = mixed.at[f, :, OWN * to + j]
                dst = out.at[j, f, :, columns]
                if d == 0:
                    pl.when(here)(
                        lambda src=src, dst=dst: pltpu.make_async_copy(
                            src, dst, recv3
                        ).start()
                    )
                    pl.when(jnp.logical_not(here))(
                        lambda src=src, dst=dst: remote(
                            src, dst, send3.at[1], recv3, (i, a)
                        ).start()
                    )
                else:
                    remote(src, dst, send3.at[0], recv3, (to, a)).start()

    for j in range(OWN):
        rest = landed.at[j, :, pl.ds(0, ROWS * (STRIPS - 1))]
        remote(rest, rest, send1.at[j], recv1.at[j], (i, s)).wait_send()
        for copy in edge_copies(j):
            copy.wait_send()
    pl.when(jnp.logical_not(mine))(
        lambda: remote(packed, own, send_obs.at[9], recv_obs, (i, s)).wait_send()
    )
    for k in range(9):
        if k != 4:
            reach_copy(k).wait_send()
    rest = region.at[:, :, pl.ds(0, OWN * (OWNERS - 1))]
    remote(rest, rest, send2, recv2, (i, s)).wait_send()
    for k in range(9):
        if k != 4:
            gram_copy(k).wait_send()
    remote(rest, rest, send3.at[0], recv3, (i, s)).wait_send()
    few = region.at[:, :, pl.ds(0, OWN)]
    pl.when(jnp.logical_not(here))(
        lambda: remote(few, few, send3.at[1], recv3, (i, s)).wait_send()
    )
    remote(out, out, send3.at[0], recv3, (i, s)).wait_recv()


def on_device(fields, counts, cells, values, errors, radius):
    hbm = pl.BlockSpec(memory_space=pltpu.HBM)
    dma = pltpu.SemaphoreType.DMA
    return pl.pallas_call(
        kernel,
        out_shape=jax.ShapeDtypeStruct(fields.shape, F32),
        in_specs=[hbm] * 6,
        out_specs=pl.BlockSpec(memory_space=pl.ANY),
        scratch_shapes=[
            pltpu.VMEM((1, OBS), jnp.int32),
            pltpu.VMEM((2, OBS), F32),
            pltpu.VMEM((1, 1), jnp.int32),
            pltpu.VMEM((1, 1), jnp.int32),
            pltpu.VMEM((OWN, 3, STRIPS * ROWS, BLOCK), F32),
            pltpu.VMEM((2, 2, 3, SPAN, COLS), F32),
            pltpu.VMEM((OWN, 2, 3, EDGE, COLS), F32),
            pltpu.VMEM((OWN, 2, 3, EDGE, COLS), F32),
            pltpu.VMEM((OWN, 3, STRIPS * ROWS, BLOCK), F32),
            pltpu.VMEM((3, ROWS, MEMBERS, COLS), F32),
            pltpu.VMEM((3, ROWS, MEMBERS, COLS), F32),
            pltpu.VMEM((8, OBS), F32),
            pltpu.VMEM((8, OBS), F32),
            pltpu.VMEM((8, COLS), F32),
            pltpu.VMEM((9, 8, COLS), F32),
            pltpu.VMEM((ROWS * COLS, OBS), BF16),
            pltpu.VMEM((OBS, COLS), BF16),
            pltpu.VMEM((OBS, COLS), BF16),
            pltpu.VMEM((2, MEMBERS, MEMBERS), F32),
            pltpu.VMEM((MEMBERS, COLS), BF16),
            pltpu.VMEM((MEMBERS, COLS), BF16),
            pltpu.VMEM((9, MEMBERS, COLS), F32),
            pltpu.VMEM((9, MEMBERS, COLS), F32),
            dma((5,)), dma((OWN,)), dma((OWN,)), dma((OWN, 2)), dma((OWN, 2)), dma, dma,
            dma((10,)), dma, dma((9,)),
            dma((9,)), dma((9,)), dma((2,)), dma,
        ],
        compiler_params=pltpu.CompilerParams(
            collective_id=0, has_side_effects=True, vmem_limit_bytes=40 * 1024 * 1024
        ),
        name="forecast_and_analysis",
    )(
        fields, cells.reshape(1, OBS), values.reshape(1, OBS), errors.reshape(1, OBS),
        counts, radius,
    )


def solution(mesh):
    in_specs = (
        P("member", None, "strip", None),
        P("strip", "member"),
        P("strip", "member", None),
        P("strip", "member", None),
        P("strip", "member", None),
        P("strip", "member"),
    )
    return jax.shard_map(
        on_device, mesh=mesh, in_specs=in_specs, out_specs=P("member", None, "strip", None),
        check_vma=False,
    )
```

```python
import jax
import jax.numpy as jnp
from jax import lax
from jax.experimental import pallas as pl
from jax.experimental.pallas import tpu as pltpu
from jax.sharding import PartitionSpec as P

STEPS = 12
TURNS = 20
MEMBERS = 64
OWN = 4
STRIPS = 8
OWNERS = 16
ROWS = 16
COLS = 128
BLOCK = 256
OBS = 256
EDGE = 16
GUARD = 8
FIRST = GUARD + EDGE
SPAN = BLOCK + 2 * EDGE + 2 * GUARD
MESH = pl.DeviceIdType.MESH
F32 = jnp.float32
BF16 = jnp.bfloat16


def region_of(i, strip):
    y, c, z = (i // 2) % 4, i % 2, strip // 2
    a = 2 * ((y + z) % 4) + (c + y) % 2
    return a, (2 * strip + i // 8 + a % 2) % OWNERS


def owner_of(a, b):
    first = (b + OWNERS - a % 2) % OWNERS
    y = (a // 2 + 4 - first // 4) % 4
    return (first % 2) * 8 + y * 2 + (a + y) % 2, first // 2


def remote(src, dst, send, recv, where):
    return pltpu.make_async_remote_copy(
        src_ref=src, dst_ref=dst, send_sem=send, recv_sem=recv, device_id=where, device_id_type=MESH
    )


def halves(value):
    high = value.astype(BF16)
    return high, (value - high.astype(F32)).astype(BF16)


def thirds(value):
    high = value.astype(BF16)
    rest = value - high.astype(F32)
    mid = rest.astype(BF16)
    return high, mid, (rest - mid.astype(F32)).astype(BF16)


def dot(a, b):
    return jnp.dot(a, b, preferred_element_type=F32)


def matmul(a, b):
    ah, al = halves(a)
    bh, bl = halves(b)
    return dot(ah, bh) + (dot(ah, bl) + dot(al, bh))


def turn_north(value):
    return pltpu.roll(value, COLS - 1, 1)


def turn_south(value):
    return pltpu.roll(value, 1, 1)


def step_rows(src, dst, at):
    rows = pl.ds(at, 8)
    east, west = pl.ds(at + 1, 8), pl.ds(at - 1, 8)
    h, p, q = src[0, rows], src[1, rows], src[2, rows]
    he, pe, qe = src[0, east], src[1, east], src[2, east]
    hw, pw, qw = src[0, west], src[1, west], src[2, west]
    a, a2, b, b2 = 0.25 - p, 0.25 + p, 0.25 - q, 0.25 + q
    pn, ps = turn_north(p), turn_south(p)
    qn, qs = turn_north(q), turn_south(q)
    hn, hs = turn_north(h), turn_south(h)
    flow = (pe - pw) + (qn - qs)
    dst[0, rows] = (
        (he * (0.25 - pe) + hw * (0.25 + pw)) + (hn * (0.25 - qn) + hs * (0.25 + qs))
    ) - (1.0 / 64.0) * flow
    dst[1, rows] = ((a * pe + a2 * pw) + (b * pn + b2 * ps)) + (0.05 * q - (he - hw))
    dst[2, rows] = ((a * qe + a2 * qw) + (b * qn + b2 * qs)) - (0.05 * p + (hn - hs))


def kernel(
    x, cells, values, errors, count, radius, out,
    raw_cells, raw, raw_scalars, raw_radius, held, landed, work, edge, edges, halo, staged, region, mixed, packed, own, reach, near, onehot, roots, mix_h, mix_l, gram,
    grams,
    load_sem, send1, recv1, send_edge, recv_edge, send2, recv2, send_obs, recv_obs, recv_reach,
    send_gram, recv_gram, send3, recv3,
):
    i = lax.axis_index("member")
    s = lax.axis_index("strip")
    a, b = region_of(i, s)
    shift = i // 8

    def neighbour(k):
        return owner_of((a + 7 + k // 3) % 8, (b + 15 + k % 3) % 16)

    to_i, to_s = owner_of(s, i)
    mine = (to_i == i) & (to_s == s)
    here = a == s
    loads = [
        pltpu.make_async_copy(cells, raw_cells, load_sem.at[0]),
        pltpu.make_async_copy(values, raw.at[0:1], load_sem.at[1]),
        pltpu.make_async_copy(errors, raw.at[1:2], load_sem.at[2]),
        pltpu.make_async_copy(count, raw_scalars, load_sem.at[3]),
        pltpu.make_async_copy(radius, raw_radius, load_sem.at[4]),
    ]
    for copy in loads:
        copy.start()
    own_input = pltpu.make_async_copy(x, held, load_sem.at[5])
    own_input.start()

    barrier = pltpu.get_barrier_semaphore()

    def greet(where):
        pl.semaphore_signal(barrier, inc=1, device_id=where, device_id_type=MESH)

    for k in range(9):
        if k != 4:
            greet(neighbour(k))
    for n in range(OWNERS):
        sender = owner_of(s, n)
        pl.when((sender[0] != i) | (sender[1] != s))(lambda sender=sender: greet(sender))
    pl.when((b != i) | (a != s))(lambda: greet((b, a)))
    for d in range(1, OWNERS):
        n = lax.rem(i + d, OWNERS)
        greet((n, ((b + OWNERS - n // 8) % OWNERS) // 2))
    for d in range(1, STRIPS):
        greet((i, lax.rem(s + d, STRIPS)))
    pl.semaphore_wait(
        barrier,
        8 + OWNERS + 1 + (OWNERS - 1) + (STRIPS - 1)
        - mine.astype(jnp.int32) - here.astype(jnp.int32),
    )

    for copy in loads:
        copy.wait()
    slots = lax.broadcasted_iota(jnp.int32, (1, OBS), 1)
    packed[0:1] = raw_cells[...].astype(F32)
    packed[1:2] = raw[0:1]
    packed[2:3] = jnp.where(slots < raw_scalars[0:1, 0:1], 1.0 / raw[1:2], 0.0)
    packed[3:4] = jnp.broadcast_to(raw_radius[0:1, 0:1].astype(F32), (1, OBS))

    @pl.when(mine)
    def _():
        pltpu.make_async_copy(packed, own, recv_obs).start()

    @pl.when(jnp.logical_not(mine))
    def _():
        remote(packed, own, send_obs.at[9], recv_obs, (to_i, to_s)).start()

    def columns_of(strip, n):
        return pl.ds(pl.multiple_of(((2 * strip + shift + n) % OWNERS) * COLS, COLS), COLS)

    strip_rows = pl.ds(pl.multiple_of(s * ROWS, ROWS), ROWS)

    def send_member(j):
        for d in range(1, STRIPS):
            to = lax.rem(s + d, STRIPS)
            for h in range(2):
                remote(
                    held.at[j, :, :, columns_of(to, h)],
                    landed.at[j, :, strip_rows, pl.ds(h * COLS, COLS)],
                    send1.at[j], recv1.at[j], (i, to),
                ).start()

    own_input.wait()
    send_member(0)
    for j in range(OWN):
        for h in range(2):
            pltpu.make_async_copy(
                x.at[j, :, :, columns_of(s, h)],
                landed.at[j, :, strip_rows, pl.ds(h * COLS, COLS)],
                recv1.at[j],
            ).start()
    lanes = lax.broadcasted_iota(jnp.int32, (ROWS, COLS), 1)

    def pack_edges(to, _):
        for f in range(3):
            joined = jnp.zeros((ROWS, COLS), F32)
            for j in range(OWN):
                both = jnp.where(
                    lanes < COLS // 2,
                    held[j, f, :, columns_of(to, 2)],
                    held[j, f, :, columns_of(to, OWNERS - 1)],
                )
                turned = pltpu.roll(both, j * 2 * EDGE + EDGE, 1)
                joined = jnp.where(lanes // (2 * EDGE) == j, turned, joined)
            edge[to, f] = joined
        return 0

    lax.fori_loop(0, STRIPS, pack_edges, 0)
    for d in range(1, STRIPS):
        to = lax.rem(s + d, STRIPS)
        remote(
            edge.at[to], edges.at[:, strip_rows], send_edge, recv_edge, (i, to)
        ).start()
    for j in range(1, OWN):
        send_member(j)
    edges[:, strip_rows] = edge[s]

    for g in range(2):
        for f in range(3):
            work[g, f, 0:GUARD] = jnp.zeros((GUARD, COLS), F32)
            work[g, f, SPAN - GUARD : SPAN] = jnp.zeros((GUARD, COLS), F32)
    ping, pong = work.at[0], work.at[1]

    def arrive(j):
        pltpu.make_async_copy(landed.at[j], landed.at[j], recv1.at[j]).wait()
        for f in range(3):
            scale = 1.0 / 64.0 if f == 0 else 0.125
            for c in range(2):
                turned = landed[j, f, :, c * COLS : (c + 1) * COLS].T * scale
                ping[f, FIRST + c * COLS : FIRST + (c + 1) * COLS] = turned

    def forecast(j):
        for f in range(3):
            low, mid, high = (2 * j) * EDGE, (2 * j + 1) * EDGE, (2 * j + 2) * EDGE
            ping[f, GUARD:FIRST] = halo[f, low:mid]
            ping[f, FIRST + BLOCK : FIRST + BLOCK + EDGE] = halo[f, mid:high]

        def sweep(src, dst):
            for n in range((SPAN - 2 * GUARD) // 8):
                step_rows(src, dst, GUARD + 8 * n)

        def two_steps(n, _):
            sweep(ping, pong)
            sweep(pong, ping)
            return 0

        lax.fori_loop(0, STEPS // 2, two_steps, 0)
        for f in range(3):
            scale = 64.0 if f == 0 else 8.0
            for c in range(2):
                block = ping[f, FIRST + c * COLS : FIRST + (c + 1) * COLS]
                staged[j, f, :, c * COLS : (c + 1) * COLS] = block.T * scale
        for d in range(STRIPS):
            to_a = lax.rem(a + d, STRIPS)
            for e in range(2):
                n = (to_a + d + e) % 2
                src = staged.at[
                    j, :, pl.ds(pl.multiple_of(to_a * ROWS, ROWS), ROWS),
                    pl.ds(pl.multiple_of(n * COLS, COLS), COLS),
                ]
                dst = region.at[:, :, OWN * i + j]
                if d == 0 and e == 0:
                    pltpu.make_async_copy(src, dst, recv2).start()
                else:
                    to = owner_of(to_a, (2 * s + shift + n) % OWNERS)
                    remote(src, dst, send2, recv2, to).start()

    def reach_copy(k):
        return remote(
            reach, near.at[k], send_obs.at[k], recv_reach.at[k], neighbour(k)
        )

    pltpu.make_async_copy(own, own, recv_obs).wait()
    reach[...] = jnp.broadcast_to(own[3:4, :COLS], (8, COLS))
    for k in range(9):
        if k != 4:
            reach_copy(k).start()
    place = own[0:1]

    def mark(n, _):
        at = pl.multiple_of(n * COLS, COLS)
        cell = lax.broadcasted_iota(jnp.int32, (COLS, OBS), 0) + at
        onehot[pl.ds(at, COLS)] = jnp.where(cell.astype(F32) == place, 1.0, 0.0).astype(BF16)
        return 0

    lax.fori_loop(0, ROWS, mark, 0)
    arrive(0)
    rest = edges.at[:, pl.ds(0, ROWS * (STRIPS - 1))]
    remote(rest, rest, send_edge, recv_edge, (i, s)).wait_recv()
    for f in range(3):
        halo[f] = edges[f].T * (1.0 / 64.0 if f == 0 else 0.125)
    forecast(0)
    for j in range(1, OWN):
        arrive(j)
        forecast(j)

    pltpu.make_async_copy(region, region, recv2).wait()

    def look(n, height):
        pair = jnp.concatenate([region[0, 2 * n], region[0, 2 * n + 1]], axis=1)
        marks = onehot[pl.ds(pl.multiple_of(n * OBS, OBS), OBS)]
        high, mid, low = thirds(pair)
        return height + (dot(high, marks) + (dot(mid, marks) + dot(low, marks)))

    height = lax.fori_loop(0, ROWS // 2, look, jnp.zeros((MEMBERS, OBS), F32))
    mean = jnp.mean(height, axis=0, keepdims=True)
    spread = height - mean
    innovation = own[1:2] - mean
    precision = own[2:3]
    line = jnp.floor(place * (1.0 / COLS))
    row_pos = (line + 0.5) * (1.0 / ROWS) - 0.5
    col_pos = (place - line * COLS + 0.5) * (1.0 / COLS) - 0.5
    wide = jnp.concatenate(
        [spread, innovation, jnp.zeros((COLS - MEMBERS - 1, OBS), F32)], axis=0
    )
    tall = jnp.concatenate([wide[:, :COLS].T, wide[:, COLS:].T], axis=0)
    columns_h, columns_l = halves(tall)
    for k in range(9):
        if k != 4:
            reach_copy(k).wait_recv()
    near[4] = reach[...]

    def gram_copy(k):
        return remote(
            gram.at[k], grams.at[k], send_gram.at[k], recv_gram.at[k], neighbour(8 - k)
        )

    for k in (0, 1, 2, 3, 5, 6, 7, 8, 4):
        r, c = row_pos + (k // 3 - 1.0), col_pos + (k % 3 - 1.0)
        radius_k = near[k, 0:1, 0:1]
        taper = jnp.exp(-0.5 * (r * r + c * c) / (radius_k * radius_k))
        wh, wl = halves(spread * (taper * precision))
        gram[k] = dot(wh, columns_h) + (dot(wh, columns_l) + dot(wl, columns_h))
        if k != 4:
            gram_copy(k).start()
    total = gram[4]
    for k in range(9):
        if k != 4:
            gram_copy(k).wait_recv()
            total = total + grams[k]

    scale = 1.0 / (MEMBERS - 1.0)
    eye = (
        lax.broadcasted_iota(jnp.int32, (MEMBERS, MEMBERS), 0)
        == lax.broadcasted_iota(jnp.int32, (MEMBERS, MEMBERS), 1)
    ).astype(F32)
    normal = eye + total[:, :MEMBERS] * scale
    frob2 = jnp.sum(jnp.sum(normal * normal, axis=1, keepdims=True), axis=0, keepdims=True)
    frob = jnp.sqrt(frob2)

    roots[0], roots[1] = normal / frob, eye

    def turn(_, carry):
        u, z = roots[0], roots[1]
        factor = 1.5 * eye - 0.5 * matmul(z, u)
        roots[0], roots[1] = matmul(u, factor), matmul(factor, z)
        return carry

    lax.fori_loop(0, TURNS, turn, 0)
    inverse = roots[1]
    pull = matmul(inverse, matmul(inverse, total)) / frob
    lane = lax.broadcasted_iota(jnp.int32, (MEMBERS, COLS), 1)
    mean_weights = jnp.sum(jnp.where(lane == MEMBERS, pull, 0.0), axis=1, keepdims=True) * scale
    transform = inverse / jnp.sqrt(frob) + mean_weights
    padded = jnp.concatenate(
        [
            jnp.concatenate([transform, jnp.zeros((MEMBERS, MEMBERS), F32)], axis=1),
            jnp.zeros((MEMBERS, COLS), F32),
        ],
        axis=0,
    )
    weights_h, weights_l = halves(padded.T[:MEMBERS])
    mix_h[...], mix_l[...] = weights_h, weights_l

    columns = pl.ds(pl.multiple_of(b * COLS, COLS), COLS)
    for f in range(3):

        def rows_of(n, _):
            pair = jnp.concatenate([region[f, 2 * n], region[f, 2 * n + 1]], axis=1)
            centre = jnp.mean(pair, axis=0, keepdims=True)
            dev_h, dev_l = halves(pair - centre)
            result = centre + (
                dot(mix_h[:, :MEMBERS], dev_h)
                + (dot(mix_h[:, :MEMBERS], dev_l) + dot(mix_l[:, :MEMBERS], dev_h))
            )
            mixed[f, 2 * n] = result[:, :COLS]
            mixed[f, 2 * n + 1] = result[:, COLS:]
            return 0

        lax.fori_loop(0, ROWS // 2, rows_of, 0)
        for d in range(OWNERS):
            to = lax.rem(i + d, OWNERS)
            for j in range(OWN):
                src = mixed.at[f, :, OWN * to + j]
                dst = out.at[j, f, :, columns]
                if d == 0:
                    pl.when(here)(
                        lambda src=src, dst=dst: pltpu.make_async_copy(
                            src, dst, recv3
                        ).start()
                    )
                    pl.when(jnp.logical_not(here))(
                        lambda src=src, dst=dst: remote(
                            src, dst, send3.at[1], recv3, (i, a)
                        ).start()
                    )
                else:
                    remote(src, dst, send3.at[0], recv3, (to, a)).start()

    for j in range(OWN):
        rest = landed.at[j, :, pl.ds(0, ROWS * (STRIPS - 1))]
        remote(rest, rest, send1.at[j], recv1.at[j], (i, s)).wait_send()
    rest = edges.at[:, pl.ds(0, ROWS * (STRIPS - 1))]
    remote(rest, rest, send_edge, recv_edge, (i, s)).wait_send()
    pl.when(jnp.logical_not(mine))(
        lambda: remote(packed, own, send_obs.at[9], recv_obs, (i, s)).wait_send()
    )
    for k in range(9):
        if k != 4:
            reach_copy(k).wait_send()
    rest = region.at[:, :, pl.ds(0, OWN * (OWNERS - 1))]
    remote(rest, rest, send2, recv2, (i, s)).wait_send()
    for k in range(9):
        if k != 4:
            gram_copy(k).wait_send()
    remote(rest, rest, send3.at[0], recv3, (i, s)).wait_send()
    few = region.at[:, :, pl.ds(0, OWN)]
    pl.when(jnp.logical_not(here))(
        lambda: remote(few, few, send3.at[1], recv3, (i, s)).wait_send()
    )
    remote(out, out, send3.at[0], recv3, (i, s)).wait_recv()


def on_device(fields, counts, cells, values, errors, radius):
    hbm = pl.BlockSpec(memory_space=pltpu.HBM)
    dma = pltpu.SemaphoreType.DMA
    return pl.pallas_call(
        kernel,
        out_shape=jax.ShapeDtypeStruct(fields.shape, F32),
        in_specs=[hbm] * 6,
        out_specs=pl.BlockSpec(memory_space=pl.ANY),
        scratch_shapes=[
            pltpu.VMEM((1, OBS), jnp.int32),
            pltpu.VMEM((2, OBS), F32),
            pltpu.VMEM((1, 1), jnp.int32),
            pltpu.VMEM((1, 1), jnp.int32),
            pltpu.VMEM((OWN, 3, ROWS, 2048), F32),
            pltpu.VMEM((OWN, 3, STRIPS * ROWS, BLOCK), F32),
            pltpu.VMEM((2, 3, SPAN, COLS), F32),
            pltpu.VMEM((STRIPS, 3, ROWS, COLS), F32),
            pltpu.VMEM((3, STRIPS * ROWS, COLS), F32),
            pltpu.VMEM((3, STRIPS * ROWS, COLS), F32),
            pltpu.VMEM((OWN, 3, STRIPS * ROWS, BLOCK), F32),
            pltpu.VMEM((3, ROWS, MEMBERS, COLS), F32),
            pltpu.VMEM((3, ROWS, MEMBERS, COLS), F32),
            pltpu.VMEM((8, OBS), F32),
            pltpu.VMEM((8, OBS), F32),
            pltpu.VMEM((8, COLS), F32),
            pltpu.VMEM((9, 8, COLS), F32),
            pltpu.VMEM((ROWS * COLS, OBS), BF16),
            pltpu.VMEM((2, MEMBERS, MEMBERS), F32),
            pltpu.VMEM((MEMBERS, COLS), BF16),
            pltpu.VMEM((MEMBERS, COLS), BF16),
            pltpu.VMEM((9, MEMBERS, COLS), F32),
            pltpu.VMEM((9, MEMBERS, COLS), F32),
            dma((6,)), dma((OWN,)), dma((OWN,)), dma, dma, dma, dma,
            dma((10,)), dma, dma((9,)),
            dma((9,)), dma((9,)), dma((2,)), dma,
        ],
        compiler_params=pltpu.CompilerParams(
            collective_id=0, has_side_effects=True, vmem_limit_bytes=67043328
        ),
        name="forecast_and_analysis",
    )(
        fields, cells.reshape(1, OBS), values.reshape(1, OBS), errors.reshape(1, OBS),
        counts, radius,
    )


def solution(mesh):
    in_specs = (
        P("member", None, "strip", None),
        P("strip", "member"),
        P("strip", "member", None),
        P("strip", "member", None),
        P("strip", "member", None),
        P("strip", "member"),
    )
    return jax.shard_map(
        on_device, mesh=mesh, in_specs=in_specs, out_specs=P("member", None, "strip", None),
        check_vma=False,
    )
```

```python
import jax
import jax.numpy as jnp
from jax import lax
from jax.experimental import pallas as pl
from jax.experimental.pallas import tpu as pltpu
from jax.sharding import PartitionSpec as P

STEPS = 12
TURNS = 20
MEMBERS = 64
OWN = 4
STRIPS = 8
OWNERS = 16
ROWS = 16
COLS = 128
BLOCK = 256
OBS = 256
EDGE = 16
GUARD = 8
FIRST = GUARD + EDGE
SPAN = BLOCK + 2 * EDGE + 2 * GUARD
MESH = pl.DeviceIdType.MESH
F32 = jnp.float32
BF16 = jnp.bfloat16


def region_of(i, strip):
    y, c, z = (i // 2) % 4, i % 2, strip // 2
    a = 2 * ((y + z) % 4) + (c + y) % 2
    return a, (2 * strip + i // 8 + a % 2) % OWNERS


def owner_of(a, b):
    first = (b + OWNERS - a % 2) % OWNERS
    y = (a // 2 + 4 - first // 4) % 4
    return (first % 2) * 8 + y * 2 + (a + y) % 2, first // 2


def remote(src, dst, send, recv, where):
    return pltpu.make_async_remote_copy(
        src_ref=src, dst_ref=dst, send_sem=send, recv_sem=recv, device_id=where, device_id_type=MESH
    )


def halves(value):
    high = value.astype(BF16)
    return high, (value - high.astype(F32)).astype(BF16)


def thirds(value):
    high = value.astype(BF16)
    rest = value - high.astype(F32)
    mid = rest.astype(BF16)
    return high, mid, (rest - mid.astype(F32)).astype(BF16)


def dot(a, b):
    return jnp.dot(a, b, preferred_element_type=F32)


def matmul(a, b):
    ah, al = halves(a)
    bh, bl = halves(b)
    return dot(ah, bh) + (dot(ah, bl) + dot(al, bh))


def turn_north(value):
    return pltpu.roll(value, COLS - 1, 1)


def turn_south(value):
    return pltpu.roll(value, 1, 1)


def step_rows(src, dst, at):
    rows = pl.ds(at, 8)
    east, west = pl.ds(at + 1, 8), pl.ds(at - 1, 8)
    h, p, q = src[0, rows], src[1, rows], src[2, rows]
    he, pe, qe = src[0, east], src[1, east], src[2, east]
    hw, pw, qw = src[0, west], src[1, west], src[2, west]
    a, a2, b, b2 = 0.25 - p, 0.25 + p, 0.25 - q, 0.25 + q
    pn, ps = turn_north(p), turn_south(p)
    qn, qs = turn_north(q), turn_south(q)
    hn, hs = turn_north(h), turn_south(h)
    flow = (pe - pw) + (qn - qs)
    dst[0, rows] = (
        (he * (0.25 - pe) + hw * (0.25 + pw)) + (hn * (0.25 - qn) + hs * (0.25 + qs))
    ) - (1.0 / 64.0) * flow
    dst[1, rows] = ((a * pe + a2 * pw) + (b * pn + b2 * ps)) + (0.05 * q - (he - hw))
    dst[2, rows] = ((a * qe + a2 * qw) + (b * qn + b2 * qs)) - (0.05 * p + (hn - hs))


def kernel(
    x, cells, values, errors, count, radius, out,
    raw_cells, raw, raw_scalars, raw_radius, held, landed, work, edge, edges, halo, staged, region, mixed, packed, own, reach, near, onehot, observed, roots, mix_h, mix_l, gram,
    grams,
    load_sem, send1, recv1, send_edge, recv_edge, send2, recv2, send_obs, recv_obs, recv_reach,
    send_gram, recv_gram, send3, recv3,
):
    i = lax.axis_index("member")
    s = lax.axis_index("strip")
    a, b = region_of(i, s)
    shift = i // 8

    def neighbour(k):
        return owner_of((a + 7 + k // 3) % 8, (b + 15 + k % 3) % 16)

    to_i, to_s = owner_of(s, i)
    mine = (to_i == i) & (to_s == s)
    here = a == s
    loads = [
        pltpu.make_async_copy(cells, raw_cells, load_sem.at[0]),
        pltpu.make_async_copy(values, raw.at[0:1], load_sem.at[1]),
        pltpu.make_async_copy(errors, raw.at[1:2], load_sem.at[2]),
        pltpu.make_async_copy(count, raw_scalars, load_sem.at[3]),
        pltpu.make_async_copy(radius, raw_radius, load_sem.at[4]),
    ]
    for copy in loads:
        copy.start()
    own_input = pltpu.make_async_copy(x, held, load_sem.at[5])
    own_input.start()

    barrier = pltpu.get_barrier_semaphore()

    def greet(where):
        pl.semaphore_signal(barrier, inc=1, device_id=where, device_id_type=MESH)

    for k in range(9):
        if k != 4:
            greet(neighbour(k))
    for n in range(OWNERS):
        sender = owner_of(s, n)
        pl.when((sender[0] != i) | (sender[1] != s))(lambda sender=sender: greet(sender))
    pl.when((b != i) | (a != s))(lambda: greet((b, a)))
    for d in range(1, OWNERS):
        n = lax.rem(i + d, OWNERS)
        greet((n, ((b + OWNERS - n // 8) % OWNERS) // 2))
    for d in range(1, STRIPS):
        greet((i, lax.rem(s + d, STRIPS)))
    pl.semaphore_wait(
        barrier,
        8 + OWNERS + 1 + (OWNERS - 1) + (STRIPS - 1)
        - mine.astype(jnp.int32) - here.astype(jnp.int32),
    )

    for copy in loads:
        copy.wait()
    slots = lax.broadcasted_iota(jnp.int32, (1, OBS), 1)
    packed[0:1] = raw_cells[...].astype(F32)
    packed[1:2] = raw[0:1]
    packed[2:3] = jnp.where(slots < raw_scalars[0:1, 0:1], 1.0 / raw[1:2], 0.0)
    packed[3:4] = jnp.broadcast_to(raw_radius[0:1, 0:1].astype(F32), (1, OBS))

    @pl.when(mine)
    def _():
        pltpu.make_async_copy(packed, own, recv_obs).start()

    @pl.when(jnp.logical_not(mine))
    def _():
        remote(packed, own, send_obs.at[9], recv_obs, (to_i, to_s)).start()

    def columns_of(strip, n):
        return pl.ds(pl.multiple_of(((2 * strip + shift + n) % OWNERS) * COLS, COLS), COLS)

    strip_rows = pl.ds(pl.multiple_of(s * ROWS, ROWS), ROWS)

    def send_member(j):
        for d in range(1, STRIPS):
            to = lax.rem(s + d, STRIPS)
            for h in range(2):
                remote(
                    held.at[j, :, :, columns_of(to, h)],
                    landed.at[j, :, strip_rows, pl.ds(h * COLS, COLS)],
                    send1.at[j], recv1.at[j], (i, to),
                ).start()

    own_input.wait()
    send_member(0)
    for j in range(OWN):
        for h in range(2):
            pltpu.make_async_copy(
                x.at[j, :, :, columns_of(s, h)],
                landed.at[j, :, strip_rows, pl.ds(h * COLS, COLS)],
                recv1.at[j],
            ).start()
    lanes = lax.broadcasted_iota(jnp.int32, (ROWS, COLS), 1)

    def pack_edges(to, _):
        for f in range(3):
            joined = jnp.zeros((ROWS, COLS), F32)
            for j in range(OWN):
                both = jnp.where(
                    lanes < COLS // 2,
                    held[j, f, :, columns_of(to, 2)],
                    held[j, f, :, columns_of(to, OWNERS - 1)],
                )
                turned = pltpu.roll(both, j * 2 * EDGE + EDGE, 1)
                joined = jnp.where(lanes // (2 * EDGE) == j, turned, joined)
            edge[to, f] = joined
        return 0

    lax.fori_loop(0, STRIPS, pack_edges, 0)
    for d in range(1, STRIPS):
        to = lax.rem(s + d, STRIPS)
        remote(
            edge.at[to], edges.at[:, strip_rows], send_edge, recv_edge, (i, to)
        ).start()
    for j in range(1, OWN):
        send_member(j)
    edges[:, strip_rows] = edge[s]

    for g in range(2):
        for f in range(3):
            work[g, f, 0:GUARD] = jnp.zeros((GUARD, COLS), F32)
            work[g, f, SPAN - GUARD : SPAN] = jnp.zeros((GUARD, COLS), F32)
    ping, pong = work.at[0], work.at[1]

    def arrive(j):
        pltpu.make_async_copy(landed.at[j], landed.at[j], recv1.at[j]).wait()
        for f in range(3):
            scale = 1.0 / 64.0 if f == 0 else 0.125
            for c in range(2):
                turned = landed[j, f, :, c * COLS : (c + 1) * COLS].T * scale
                ping[f, FIRST + c * COLS : FIRST + (c + 1) * COLS] = turned

    def forecast(j):
        for f in range(3):
            low, mid, high = (2 * j) * EDGE, (2 * j + 1) * EDGE, (2 * j + 2) * EDGE
            ping[f, GUARD:FIRST] = halo[f, low:mid]
            ping[f, FIRST + BLOCK : FIRST + BLOCK + EDGE] = halo[f, mid:high]

        def sweep(src, dst):
            for n in range((SPAN - 2 * GUARD) // 8):
                step_rows(src, dst, GUARD + 8 * n)

        def two_steps(n, _):
            sweep(ping, pong)
            sweep(pong, ping)
            return 0

        lax.fori_loop(0, STEPS // 2, two_steps, 0)
        for f in range(3):
            scale = 64.0 if f == 0 else 8.0
            for c in range(2):
                block = ping[f, FIRST + c * COLS : FIRST + (c + 1) * COLS]
                staged[j, f, :, c * COLS : (c + 1) * COLS] = block.T * scale

    def send_fields(j, low, high):
        for d in range(STRIPS):
            to_a = lax.rem(a + d, STRIPS)
            for e in range(2):
                n = (to_a + d + e) % 2
                src = staged.at[
                    j, low:high, pl.ds(pl.multiple_of(to_a * ROWS, ROWS), ROWS),
                    pl.ds(pl.multiple_of(n * COLS, COLS), COLS),
                ]
                dst = region.at[low:high, :, OWNERS * j + i]
                done = recv2.at[j if low == 0 else OWN]
                if d == 0 and e == 0:
                    pltpu.make_async_copy(src, dst, done).start()
                else:
                    to = owner_of(to_a, (2 * s + shift + n) % OWNERS)
                    remote(src, dst, send2, done, to).start()

    def reach_copy(k):
        return remote(
            reach, near.at[k], send_obs.at[k], recv_reach.at[k], neighbour(k)
        )

    pltpu.make_async_copy(own, own, recv_obs).wait()
    reach[...] = jnp.broadcast_to(own[3:4, :COLS], (8, COLS))
    for k in range(9):
        if k != 4:
            reach_copy(k).start()
    place = own[0:1]

    def mark(n, _):
        at = pl.multiple_of(n * COLS, COLS)
        cell = lax.broadcasted_iota(jnp.int32, (COLS, OBS), 0) + at
        onehot[pl.ds(at, COLS)] = jnp.where(cell.astype(F32) == place, 1.0, 0.0).astype(BF16)
        return 0

    lax.fori_loop(0, ROWS, mark, 0)
    arrive(0)
    rest = edges.at[:, pl.ds(0, ROWS * (STRIPS - 1))]
    remote(rest, rest, send_edge, recv_edge, (i, s)).wait_recv()
    for f in range(3):
        halo[f] = edges[f].T * (1.0 / 64.0 if f == 0 else 0.125)
    forecast(0)
    send_fields(0, 0, 1)
    send_fields(0, 1, 3)
    arrive(1)
    forecast(1)
    send_fields(1, 0, 1)
    send_fields(1, 1, 3)
    arrive(2)
    forecast(2)
    send_fields(2, 0, 1)
    arrive(3)
    forecast(3)
    send_fields(3, 0, 1)

    for j in range(OWN):
        group = slice(OWNERS * j, OWNERS * (j + 1))
        some = region.at[0, :, group]
        pltpu.make_async_copy(some, some, recv2.at[j]).wait()
        found = jnp.zeros((OWNERS, OBS), F32)
        for n in range(8):
            pair = jnp.concatenate(
                [region[0, 2 * n, group], region[0, 2 * n + 1, group]], axis=1
            )
            marks = onehot[n * OBS : (n + 1) * OBS]
            part = dot(jnp.concatenate(thirds(pair), axis=0), marks)
            found = found + (
                part[:OWNERS] + (part[OWNERS : 2 * OWNERS] + part[2 * OWNERS :])
            )
        observed[group] = found
    height = observed[...]
    mean = jnp.mean(height, axis=0, keepdims=True)
    spread = height - mean
    innovation = own[1:2] - mean
    precision = own[2:3]
    line = jnp.floor(place * (1.0 / COLS))
    row_pos = (line + 0.5) * (1.0 / ROWS) - 0.5
    col_pos = (place - line * COLS + 0.5) * (1.0 / COLS) - 0.5
    wide = jnp.concatenate(
        [spread, innovation, jnp.zeros((COLS - MEMBERS - 1, OBS), F32)], axis=0
    )
    tall = jnp.concatenate([wide[:, :COLS].T, wide[:, COLS:].T], axis=0)
    columns_h, columns_l = halves(tall)
    for k in range(9):
        if k != 4:
            reach_copy(k).wait_recv()
    near[4] = reach[...]

    def gram_copy(k):
        return remote(
            gram.at[k], grams.at[k], send_gram.at[k], recv_gram.at[k], neighbour(8 - k)
        )

    weighted_h, weighted_l = [], []
    for k in range(9):
        r, c = row_pos + (k // 3 - 1.0), col_pos + (k % 3 - 1.0)
        radius_k = near[k, 0:1, 0:1]
        taper = jnp.exp(-0.5 * (r * r + c * c) / (radius_k * radius_k))
        wh, wl = halves(spread * (taper * precision))
        weighted_h.append(wh)
        weighted_l.append(wl)
    weighted_h = jnp.concatenate(weighted_h, axis=0)
    weighted_l = jnp.concatenate(weighted_l, axis=0)
    products = dot(weighted_h, columns_h) + (
        dot(weighted_h, columns_l) + dot(weighted_l, columns_h)
    )
    for k in range(9):
        gram[k] = products[k * MEMBERS : (k + 1) * MEMBERS]
    for k in range(9):
        if k != 4:
            gram_copy(k).start()
    send_fields(2, 1, 3)
    send_fields(3, 1, 3)
    total = gram[4]
    for k in range(9):
        if k != 4:
            gram_copy(k).wait_recv()
            total = total + grams[k]

    scale = 1.0 / (MEMBERS - 1.0)
    eye = (
        lax.broadcasted_iota(jnp.int32, (MEMBERS, MEMBERS), 0)
        == lax.broadcasted_iota(jnp.int32, (MEMBERS, MEMBERS), 1)
    ).astype(F32)
    normal = eye + total[:, :MEMBERS] * scale
    frob2 = jnp.sum(jnp.sum(normal * normal, axis=1, keepdims=True), axis=0, keepdims=True)
    frob = jnp.sqrt(frob2)

    roots[0], roots[1] = normal / frob, eye

    def turn(_, carry):
        u, z = roots[0], roots[1]
        factor = 1.5 * eye - 0.5 * matmul(z, u)
        roots[0], roots[1] = matmul(u, factor), matmul(factor, z)
        return carry

    lax.fori_loop(0, TURNS, turn, 0)
    inverse = roots[1]
    pull = matmul(inverse, matmul(inverse, total)) / frob
    lane = lax.broadcasted_iota(jnp.int32, (MEMBERS, COLS), 1)
    mean_weights = jnp.sum(jnp.where(lane == MEMBERS, pull, 0.0), axis=1, keepdims=True) * scale
    transform = inverse / jnp.sqrt(frob) + mean_weights
    padded = jnp.concatenate(
        [
            jnp.concatenate([transform, jnp.zeros((MEMBERS, MEMBERS), F32)], axis=1),
            jnp.zeros((MEMBERS, COLS), F32),
        ],
        axis=0,
    )
    weights_h, weights_l = halves(padded.T[:MEMBERS])
    mix_h[...], mix_l[...] = weights_h, weights_l

    columns = pl.ds(pl.multiple_of(b * COLS, COLS), COLS)
    flows = region.at[1:3]
    for f in range(3):
        if f == 1:
            pltpu.make_async_copy(flows, flows, recv2.at[OWN]).wait()

        def rows_of(n, _):
            pair = jnp.concatenate([region[f, 2 * n], region[f, 2 * n + 1]], axis=1)
            centre = jnp.mean(pair, axis=0, keepdims=True)
            dev_h, dev_l = halves(pair - centre)
            result = centre + (
                dot(mix_h[:, :MEMBERS], dev_h)
                + (dot(mix_h[:, :MEMBERS], dev_l) + dot(mix_l[:, :MEMBERS], dev_h))
            )
            mixed[f, 2 * n] = result[:, :COLS]
            mixed[f, 2 * n + 1] = result[:, COLS:]
            return 0

        lax.fori_loop(0, ROWS // 2, rows_of, 0)
        for d in range(OWNERS):
            to = lax.rem(i + d, OWNERS)
            for j in range(OWN):
                src = mixed.at[f, :, OWNERS * j + to]
                dst = out.at[j, f, :, columns]
                if d == 0:
                    pl.when(here)(
                        lambda src=src, dst=dst: pltpu.make_async_copy(
                            src, dst, recv3
                        ).start()
                    )
                    pl.when(jnp.logical_not(here))(
                        lambda src=src, dst=dst: remote(
                            src, dst, send3.at[1], recv3, (i, a)
                        ).start()
                    )
                else:
                    remote(src, dst, send3.at[0], recv3, (to, a)).start()

    for j in range(OWN):
        rest = landed.at[j, :, pl.ds(0, ROWS * (STRIPS - 1))]
        remote(rest, rest, send1.at[j], recv1.at[j], (i, s)).wait_send()
    rest = edges.at[:, pl.ds(0, ROWS * (STRIPS - 1))]
    remote(rest, rest, send_edge, recv_edge, (i, s)).wait_send()
    pl.when(jnp.logical_not(mine))(
        lambda: remote(packed, own, send_obs.at[9], recv_obs, (i, s)).wait_send()
    )
    for k in range(9):
        if k != 4:
            reach_copy(k).wait_send()
    rest = region.at[:, :, pl.ds(0, OWN * (OWNERS - 1))]
    remote(rest, rest, send2, recv2.at[0], (i, s)).wait_send()
    for k in range(9):
        if k != 4:
            gram_copy(k).wait_send()
    remote(rest, rest, send3.at[0], recv3, (i, s)).wait_send()
    few = region.at[:, :, pl.ds(0, OWN)]
    pl.when(jnp.logical_not(here))(
        lambda: remote(few, few, send3.at[1], recv3, (i, s)).wait_send()
    )
    remote(out, out, send3.at[0], recv3, (i, s)).wait_recv()


def on_device(fields, counts, cells, values, errors, radius):
    hbm = pl.BlockSpec(memory_space=pltpu.HBM)
    dma = pltpu.SemaphoreType.DMA
    return pl.pallas_call(
        kernel,
        out_shape=jax.ShapeDtypeStruct(fields.shape, F32),
        in_specs=[hbm] * 6,
        out_specs=pl.BlockSpec(memory_space=pl.ANY),
        scratch_shapes=[
            pltpu.VMEM((1, OBS), jnp.int32),
            pltpu.VMEM((2, OBS), F32),
            pltpu.VMEM((1, 1), jnp.int32),
            pltpu.VMEM((1, 1), jnp.int32),
            pltpu.VMEM((OWN, 3, ROWS, 2048), F32),
            pltpu.VMEM((OWN, 3, STRIPS * ROWS, BLOCK), F32),
            pltpu.VMEM((2, 3, SPAN, COLS), F32),
            pltpu.VMEM((STRIPS, 3, ROWS, COLS), F32),
            pltpu.VMEM((3, STRIPS * ROWS, COLS), F32),
            pltpu.VMEM((3, STRIPS * ROWS, COLS), F32),
            pltpu.VMEM((OWN, 3, STRIPS * ROWS, BLOCK), F32),
            pltpu.VMEM((3, ROWS, MEMBERS, COLS), F32),
            pltpu.VMEM((3, ROWS, MEMBERS, COLS), F32),
            pltpu.VMEM((8, OBS), F32),
            pltpu.VMEM((8, OBS), F32),
            pltpu.VMEM((8, COLS), F32),
            pltpu.VMEM((9, 8, COLS), F32),
            pltpu.VMEM((ROWS * COLS, OBS), BF16),
            pltpu.VMEM((MEMBERS, OBS), F32),
            pltpu.VMEM((2, MEMBERS, MEMBERS), F32),
            pltpu.VMEM((MEMBERS, COLS), BF16),
            pltpu.VMEM((MEMBERS, COLS), BF16),
            pltpu.VMEM((9, MEMBERS, COLS), F32),
            pltpu.VMEM((9, MEMBERS, COLS), F32),
            dma((6,)), dma((OWN,)), dma((OWN,)), dma, dma, dma, dma((OWN + 1,)),
            dma((10,)), dma, dma((9,)),
            dma((9,)), dma((9,)), dma((2,)), dma,
        ],
        compiler_params=pltpu.CompilerParams(
            collective_id=0, has_side_effects=True, vmem_limit_bytes=40 * 1024 * 1024
        ),
        name="forecast_and_analysis",
    )(
        *(
            pltpu.with_memory_space_constraint(operand, pltpu.HBM)
            for operand in (
                fields, cells.reshape(1, OBS), values.reshape(1, OBS), errors.reshape(1, OBS),
            )
        ),
        counts, radius,
    )


def solution(mesh):
    in_specs = (
        P("member", None, "strip", None),
        P("strip", "member"),
        P("strip", "member", None),
        P("strip", "member", None),
        P("strip", "member", None),
        P("strip", "member"),
    )
    return jax.shard_map(
        on_device, mesh=mesh, in_specs=in_specs, out_specs=P("member", None, "strip", None),
        check_vma=False,
    )
```

```python
import jax
import jax.numpy as jnp
from jax import lax
from jax.experimental import pallas as pl
from jax.experimental.pallas import tpu as pltpu
from jax.sharding import PartitionSpec as P

STEPS = 12
TURNS = 20
MEMBERS = 64
HALF = MEMBERS // 2
OWN = 4
STRIPS = 8
OWNERS = 16
ROWS = 16
COLS = 128
BLOCK = 256
OBS = 256
EDGE = 16
GUARD = 8
FIRST = GUARD + EDGE
SPAN = BLOCK + 2 * EDGE + 2 * GUARD
MESH = pl.DeviceIdType.MESH
F32 = jnp.float32
BF16 = jnp.bfloat16


def region_of(i, strip):
    y, c, z = (i // 2) % 4, i % 2, strip // 2
    a = 2 * ((y + z) % 4) + (c + y) % 2
    return a, (2 * strip + i // 8 + a % 2) % OWNERS


def owner_of(a, b):
    first = (b + OWNERS - a % 2) % OWNERS
    y = (a // 2 + 4 - first // 4) % 4
    return (first % 2) * 8 + y * 2 + (a + y) % 2, first // 2


def remote(src, dst, send, recv, where):
    return pltpu.make_async_remote_copy(
        src_ref=src, dst_ref=dst, send_sem=send, recv_sem=recv, device_id=where, device_id_type=MESH
    )


def halves(value):
    high = value.astype(BF16)
    return high, (value - high.astype(F32)).astype(BF16)


def thirds(value):
    high = value.astype(BF16)
    rest = value - high.astype(F32)
    mid = rest.astype(BF16)
    return high, mid, (rest - mid.astype(F32)).astype(BF16)


def dot(a, b):
    return jnp.dot(a, b, preferred_element_type=F32)


def matmul(a, b):
    ah, al = halves(a)
    bh, bl = halves(b)
    return dot(ah, bh) + (dot(ah, bl) + dot(al, bh))


def turn_north(value):
    return pltpu.roll(value, COLS - 1, 1)


def turn_south(value):
    return pltpu.roll(value, 1, 1)


def step_rows(src, dst, at):
    rows = pl.ds(at, 8)
    east, west = pl.ds(at + 1, 8), pl.ds(at - 1, 8)
    h, p, q = src[0, rows], src[1, rows], src[2, rows]
    he, pe, qe = src[0, east], src[1, east], src[2, east]
    hw, pw, qw = src[0, west], src[1, west], src[2, west]
    a, a2, b, b2 = 0.25 - p, 0.25 + p, 0.25 - q, 0.25 + q
    pn, ps = turn_north(p), turn_south(p)
    qn, qs = turn_north(q), turn_south(q)
    hn, hs = turn_north(h), turn_south(h)
    flow = (pe - pw) + (qn - qs)
    dst[0, rows] = (
        (he * (0.25 - pe) + hw * (0.25 + pw)) + (hn * (0.25 - qn) + hs * (0.25 + qs))
    ) - (1.0 / 64.0) * flow
    dst[1, rows] = ((a * pe + a2 * pw) + (b * pn + b2 * ps)) + (0.05 * q - (he - hw))
    dst[2, rows] = ((a * qe + a2 * qw) + (b * qn + b2 * qs)) - (0.05 * p + (hn - hs))


def kernel(
    x, cells, values, errors, count, radius, out,
    raw_cells, raw, raw_scalars, raw_radius, held, landed, work, edge, edges, halo, staged, region, mixed, packed, own, reach, near, onehot, observed, roots, mix_h, mix_l, gram,
    grams,
    load_sem, send1, recv1, send_edge, recv_edge, send2, recv2, send_obs, recv_obs, recv_reach,
    send_gram, recv_gram, send3, recv3,
):
    i = lax.axis_index("member")
    s = lax.axis_index("strip")
    a, b = region_of(i, s)
    shift = i // 8

    def neighbour(k):
        return owner_of((a + 7 + k // 3) % 8, (b + 15 + k % 3) % 16)

    to_i, to_s = owner_of(s, i)
    mine = (to_i == i) & (to_s == s)
    here = a == s
    loads = [
        pltpu.make_async_copy(cells, raw_cells, load_sem.at[0]),
        pltpu.make_async_copy(values, raw.at[0:1], load_sem.at[1]),
        pltpu.make_async_copy(errors, raw.at[1:2], load_sem.at[2]),
        pltpu.make_async_copy(count, raw_scalars, load_sem.at[3]),
        pltpu.make_async_copy(radius, raw_radius, load_sem.at[4]),
    ]
    for copy in loads:
        copy.start()
    own_input = pltpu.make_async_copy(x, held, load_sem.at[5])
    own_input.start()

    barrier = pltpu.get_barrier_semaphore()

    def greet(where):
        pl.semaphore_signal(barrier, inc=1, device_id=where, device_id_type=MESH)

    for k in range(9):
        if k != 4:
            greet(neighbour(k))
    for n in range(OWNERS):
        sender = owner_of(s, n)
        pl.when((sender[0] != i) | (sender[1] != s))(lambda sender=sender: greet(sender))
    pl.when((b != i) | (a != s))(lambda: greet((b, a)))
    for d in range(1, OWNERS):
        n = lax.rem(i + d, OWNERS)
        greet((n, ((b + OWNERS - n // 8) % OWNERS) // 2))
    for d in range(1, STRIPS):
        greet((i, lax.rem(s + d, STRIPS)))
    pl.semaphore_wait(
        barrier,
        8 + OWNERS + 1 + (OWNERS - 1) + (STRIPS - 1)
        - mine.astype(jnp.int32) - here.astype(jnp.int32),
    )

    for copy in loads:
        copy.wait()
    slots = lax.broadcasted_iota(jnp.int32, (1, OBS), 1)
    packed[0:1] = raw_cells[...].astype(F32)
    packed[1:2] = raw[0:1]
    packed[2:3] = jnp.where(slots < raw_scalars[0:1, 0:1], 1.0 / raw[1:2], 0.0)
    packed[3:4] = jnp.broadcast_to(raw_radius[0:1, 0:1].astype(F32), (1, OBS))

    @pl.when(mine)
    def _():
        pltpu.make_async_copy(packed, own, recv_obs).start()

    @pl.when(jnp.logical_not(mine))
    def _():
        remote(packed, own, send_obs.at[9], recv_obs, (to_i, to_s)).start()

    def columns_of(strip, n):
        return pl.ds(pl.multiple_of(((2 * strip + shift + n) % OWNERS) * COLS, COLS), COLS)

    strip_rows = pl.ds(pl.multiple_of(s * ROWS, ROWS), ROWS)

    def send_member(j):
        for d in range(1, STRIPS):
            to = lax.rem(s + d, STRIPS)
            for h in range(2):
                remote(
                    held.at[j, :, :, columns_of(to, h)],
                    landed.at[j, :, strip_rows, pl.ds(h * COLS, COLS)],
                    send1.at[j], recv1.at[j], (i, to),
                ).start()

    own_input.wait()
    send_member(0)
    for j in range(OWN):
        for h in range(2):
            pltpu.make_async_copy(
                x.at[j, :, :, columns_of(s, h)],
                landed.at[j, :, strip_rows, pl.ds(h * COLS, COLS)],
                recv1.at[j],
            ).start()
    lanes = lax.broadcasted_iota(jnp.int32, (ROWS, COLS), 1)

    def pack_edges(to, _):
        for f in range(3):
            joined = jnp.zeros((ROWS, COLS), F32)
            for j in range(OWN):
                both = jnp.where(
                    lanes < COLS // 2,
                    held[j, f, :, columns_of(to, 2)],
                    held[j, f, :, columns_of(to, OWNERS - 1)],
                )
                turned = pltpu.roll(both, j * 2 * EDGE + EDGE, 1)
                joined = jnp.where(lanes // (2 * EDGE) == j, turned, joined)
            edge[to, f] = joined
        return 0

    lax.fori_loop(0, STRIPS, pack_edges, 0)
    for d in range(1, STRIPS):
        to = lax.rem(s + d, STRIPS)
        remote(
            edge.at[to], edges.at[:, strip_rows], send_edge, recv_edge, (i, to)
        ).start()
    for j in range(1, OWN):
        send_member(j)
    edges[:, strip_rows] = edge[s]

    for g in range(2):
        for f in range(3):
            work[g, f, 0:GUARD] = jnp.zeros((GUARD, COLS), F32)
            work[g, f, SPAN - GUARD : SPAN] = jnp.zeros((GUARD, COLS), F32)
    ping, pong = work.at[0], work.at[1]

    def arrive(j):
        pltpu.make_async_copy(landed.at[j], landed.at[j], recv1.at[j]).wait()
        for f in range(3):
            scale = 1.0 / 64.0 if f == 0 else 0.125
            for c in range(2):
                turned = landed[j, f, :, c * COLS : (c + 1) * COLS].T * scale
                ping[f, FIRST + c * COLS : FIRST + (c + 1) * COLS] = turned

    def send_fields(j, low, high):
        for d in range(STRIPS):
            to_a = lax.rem(a + d, STRIPS)
            for e in range(2):
                n = (to_a + d + e) % 2
                src = staged.at[
                    j, low:high, pl.ds(pl.multiple_of(to_a * ROWS, ROWS), ROWS),
                    pl.ds(pl.multiple_of(n * COLS, COLS), COLS),
                ]
                dst = region.at[low:high, :, OWNERS * j + i]
                done = recv2.at[j if low == 0 else OWN]
                if d == 0 and e == 0:
                    pltpu.make_async_copy(src, dst, done).start()
                else:
                    to = owner_of(to_a, (2 * s + shift + n) % OWNERS)
                    remote(src, dst, send2, done, to).start()

    def forecast(j):
        for f in range(3):
            low, mid, high = (2 * j) * EDGE, (2 * j + 1) * EDGE, (2 * j + 2) * EDGE
            ping[f, GUARD:FIRST] = halo[f, low:mid]
            ping[f, FIRST + BLOCK : FIRST + BLOCK + EDGE] = halo[f, mid:high]

        def sweep(src, dst):
            for n in range((SPAN - 2 * GUARD) // 8):
                step_rows(src, dst, GUARD + 8 * n)

        def two_steps(n, _):
            sweep(ping, pong)
            sweep(pong, ping)
            return 0

        lax.fori_loop(0, STEPS // 2, two_steps, 0)
        for f in range(3):
            scale = 64.0 if f == 0 else 8.0
            for c in range(2):
                block = ping[f, FIRST + c * COLS : FIRST + (c + 1) * COLS]
                staged[j, f, :, c * COLS : (c + 1) * COLS] = block.T * scale
            if f == 0:
                send_fields(j, 0, 1)

    def reach_copy(k):
        return remote(
            reach, near.at[k], send_obs.at[k], recv_reach.at[k], neighbour(k)
        )

    pltpu.make_async_copy(own, own, recv_obs).wait()
    reach[...] = jnp.broadcast_to(own[3:4, :COLS], (8, COLS))
    for k in range(9):
        if k != 4:
            reach_copy(k).start()
    place = own[0:1]

    def mark(n, _):
        at = pl.multiple_of(n * COLS, COLS)
        cell = lax.broadcasted_iota(jnp.int32, (COLS, OBS), 0) + at
        onehot[pl.ds(at, COLS)] = jnp.where(cell.astype(F32) == place, 1.0, 0.0).astype(BF16)
        return 0

    lax.fori_loop(0, ROWS, mark, 0)
    arrive(0)
    rest = edges.at[:, pl.ds(0, ROWS * (STRIPS - 1))]
    remote(rest, rest, send_edge, recv_edge, (i, s)).wait_recv()
    for f in range(3):
        halo[f] = edges[f].T * (1.0 / 64.0 if f == 0 else 0.125)
    forecast(0)
    send_fields(0, 1, 3)
    arrive(1)
    forecast(1)
    send_fields(1, 1, 3)
    arrive(2)
    forecast(2)
    arrive(3)
    forecast(3)

    for j in range(OWN):
        group = slice(OWNERS * j, OWNERS * (j + 1))
        some = region.at[0, :, group]
        pltpu.make_async_copy(some, some, recv2.at[j]).wait()
        found = jnp.zeros((OWNERS, OBS), F32)
        for n in range(8):
            pair = jnp.concatenate(
                [region[0, 2 * n, group], region[0, 2 * n + 1, group]], axis=1
            )
            marks = onehot[n * OBS : (n + 1) * OBS]
            part = dot(jnp.concatenate(thirds(pair), axis=0), marks)
            found = found + (
                part[:OWNERS] + (part[OWNERS : 2 * OWNERS] + part[2 * OWNERS :])
            )
        observed[group] = found
    height = observed[...]
    mean = jnp.mean(height, axis=0, keepdims=True)
    spread = height - mean
    innovation = own[1:2] - mean
    precision = own[2:3]
    line = jnp.floor(place * (1.0 / COLS))
    row_pos = (line + 0.5) * (1.0 / ROWS) - 0.5
    col_pos = (place - line * COLS + 0.5) * (1.0 / COLS) - 0.5
    wide = jnp.concatenate([spread, jnp.zeros((COLS - MEMBERS, OBS), F32)], axis=0)
    tall = jnp.concatenate([wide[:, :COLS].T, wide[:, COLS:].T], axis=0)
    columns_h, columns_l = halves(tall)
    for k in range(9):
        if k != 4:
            reach_copy(k).wait_recv()
    near[4] = reach[...]

    def gram_copy(k):
        return remote(
            gram.at[k], grams.at[k], send_gram.at[k], recv_gram.at[k], neighbour(8 - k)
        )

    weighted_h, weighted_l, pulls = [], [], []
    for k in range(9):
        r, c = row_pos + (k // 3 - 1.0), col_pos + (k % 3 - 1.0)
        radius_k = near[k, 0:1, 0:1]
        taper = jnp.exp(-0.5 * (r * r + c * c) / (radius_k * radius_k))
        weight = taper * precision
        wh, wl = halves(spread * weight)
        weighted_h.append(wh)
        weighted_l.append(wl)
        pulls.append(innovation * weight)
    wh, wl = halves(jnp.concatenate(pulls + [jnp.zeros((7, OBS), F32)], axis=0))
    weighted_h.append(wh)
    weighted_l.append(wl)
    weighted_h = jnp.concatenate(weighted_h, axis=0)
    weighted_l = jnp.concatenate(weighted_l, axis=0)
    products = dot(weighted_h, columns_h) + (
        dot(weighted_h, columns_l) + dot(weighted_l, columns_h)
    )
    for k in range(9):
        at = k * MEMBERS
        gram[k, :HALF] = products[at : at + HALF] + pltpu.roll(
            products[at + HALF : at + MEMBERS], MEMBERS, 1
        )
        gram[k, HALF:] = jnp.broadcast_to(
            products[9 * MEMBERS + k : 9 * MEMBERS + k + 1], (8, COLS)
        )
    for k in range(9):
        if k != 4:
            gram_copy(k).start()
    send_fields(2, 1, 3)
    send_fields(3, 1, 3)
    total = gram[4]
    for k in range(9):
        if k != 4:
            gram_copy(k).wait_recv()
            total = total + grams[k]

    scale = 1.0 / (MEMBERS - 1.0)
    eye = (
        lax.broadcasted_iota(jnp.int32, (MEMBERS, MEMBERS), 0)
        == lax.broadcasted_iota(jnp.int32, (MEMBERS, MEMBERS), 1)
    ).astype(F32)
    upper = total[:HALF]
    lower = pltpu.roll(upper, MEMBERS, 1)
    normal = eye + jnp.concatenate([upper[:, :MEMBERS], lower[:, :MEMBERS]], axis=0) * scale
    frob2 = jnp.sum(jnp.sum(normal * normal, axis=1, keepdims=True), axis=0, keepdims=True)
    frob = jnp.sqrt(frob2)

    roots[0], roots[1] = normal / frob, eye

    def turn(_, carry):
        u, z = roots[0], roots[1]
        factor = 1.5 * eye - 0.5 * matmul(z, u)
        roots[0], roots[1] = matmul(u, factor), matmul(factor, z)
        return carry

    lax.fori_loop(0, TURNS, turn, 0)
    inverse = roots[1]
    padded = jnp.concatenate(
        [
            jnp.concatenate([inverse, jnp.zeros((MEMBERS, MEMBERS), F32)], axis=1),
            jnp.zeros((MEMBERS, COLS), F32),
        ],
        axis=0,
    )
    turned = padded.T[:MEMBERS, :MEMBERS]
    pull = matmul(matmul(total[HALF:, :MEMBERS], turned), turned) / frob
    weights_h, weights_l = halves(turned / jnp.sqrt(frob) + pull[0:1] * scale)
    mix_h[...], mix_l[...] = weights_h, weights_l

    columns = pl.ds(pl.multiple_of(b * COLS, COLS), COLS)
    flows = region.at[1:3]
    for f in range(3):
        if f == 1:
            pltpu.make_async_copy(flows, flows, recv2.at[OWN]).wait()

        def rows_of(n, _):
            pair = jnp.concatenate([region[f, 2 * n], region[f, 2 * n + 1]], axis=1)
            centre = jnp.mean(pair, axis=0, keepdims=True)
            dev_h, dev_l = halves(pair - centre)
            result = centre + (
                dot(mix_h[...], dev_h)
                + (dot(mix_h[...], dev_l) + dot(mix_l[...], dev_h))
            )
            mixed[f, 2 * n] = result[:, :COLS]
            mixed[f, 2 * n + 1] = result[:, COLS:]
            return 0

        lax.fori_loop(0, ROWS // 2, rows_of, 0)
        if f == 1:
            continue
        low, high = (0, 1) if f == 0 else (1, 3)
        for d in range(OWNERS):
            to = lax.rem(i + d, OWNERS)
            for j in range(OWN):
                src = mixed.at[low:high, :, OWNERS * j + to]
                dst = out.at[j, low:high, :, columns]
                if d == 0:
                    pl.when(here)(
                        lambda src=src, dst=dst: pltpu.make_async_copy(
                            src, dst, recv3
                        ).start()
                    )
                    pl.when(jnp.logical_not(here))(
                        lambda src=src, dst=dst: remote(
                            src, dst, send3.at[1], recv3, (i, a)
                        ).start()
                    )
                else:
                    remote(src, dst, send3.at[0], recv3, (to, a)).start()

    for j in range(OWN):
        rest = landed.at[j, :, pl.ds(0, ROWS * (STRIPS - 1))]
        remote(rest, rest, send1.at[j], recv1.at[j], (i, s)).wait_send()
    rest = edges.at[:, pl.ds(0, ROWS * (STRIPS - 1))]
    remote(rest, rest, send_edge, recv_edge, (i, s)).wait_send()
    pl.when(jnp.logical_not(mine))(
        lambda: remote(packed, own, send_obs.at[9], recv_obs, (i, s)).wait_send()
    )
    for k in range(9):
        if k != 4:
            reach_copy(k).wait_send()
    rest = region.at[:, :, pl.ds(0, OWN * (OWNERS - 1))]
    remote(rest, rest, send2, recv2.at[0], (i, s)).wait_send()
    for k in range(9):
        if k != 4:
            gram_copy(k).wait_send()
    remote(rest, rest, send3.at[0], recv3, (i, s)).wait_send()
    few = region.at[:, :, pl.ds(0, OWN)]
    pl.when(jnp.logical_not(here))(
        lambda: remote(few, few, send3.at[1], recv3, (i, s)).wait_send()
    )
    remote(out, out, send3.at[0], recv3, (i, s)).wait_recv()


def on_device(fields, counts, cells, values, errors, radius):
    hbm = pl.BlockSpec(memory_space=pltpu.HBM)
    dma = pltpu.SemaphoreType.DMA
    return pl.pallas_call(
        kernel,
        out_shape=jax.ShapeDtypeStruct(fields.shape, F32),
        in_specs=[hbm] * 6,
        out_specs=pl.BlockSpec(memory_space=pl.ANY),
        scratch_shapes=[
            pltpu.VMEM((1, OBS), jnp.int32),
            pltpu.VMEM((2, OBS), F32),
            pltpu.VMEM((1, 1), jnp.int32),
            pltpu.VMEM((1, 1), jnp.int32),
            pltpu.VMEM((OWN, 3, ROWS, 2048), F32),
            pltpu.VMEM((OWN, 3, STRIPS * ROWS, BLOCK), F32),
            pltpu.VMEM((2, 3, SPAN, COLS), F32),
            pltpu.VMEM((STRIPS, 3, ROWS, COLS), F32),
            pltpu.VMEM((3, STRIPS * ROWS, COLS), F32),
            pltpu.VMEM((3, STRIPS * ROWS, COLS), F32),
            pltpu.VMEM((OWN, 3, STRIPS * ROWS, BLOCK), F32),
            pltpu.VMEM((3, ROWS, MEMBERS, COLS), F32),
            pltpu.VMEM((3, ROWS, MEMBERS, COLS), F32),
            pltpu.VMEM((8, OBS), F32),
            pltpu.VMEM((8, OBS), F32),
            pltpu.VMEM((8, COLS), F32),
            pltpu.VMEM((9, 8, COLS), F32),
            pltpu.VMEM((ROWS * COLS, OBS), BF16),
            pltpu.VMEM((MEMBERS, OBS), F32),
            pltpu.VMEM((2, MEMBERS, MEMBERS), F32),
            pltpu.VMEM((MEMBERS, MEMBERS), BF16),
            pltpu.VMEM((MEMBERS, MEMBERS), BF16),
            pltpu.VMEM((9, HALF + 8, COLS), F32),
            pltpu.VMEM((9, HALF + 8, COLS), F32),
            dma((6,)), dma((OWN,)), dma((OWN,)), dma, dma, dma, dma((OWN + 1,)),
            dma((10,)), dma, dma((9,)),
            dma((9,)), dma((9,)), dma((2,)), dma,
        ],
        compiler_params=pltpu.CompilerParams(
            collective_id=0, has_side_effects=True, vmem_limit_bytes=40 * 1024 * 1024
        ),
        name="forecast_and_analysis",
    )(
        *(
            pltpu.with_memory_space_constraint(operand, pltpu.HBM)
            for operand in (
                fields, cells.reshape(1, OBS), values.reshape(1, OBS), errors.reshape(1, OBS),
            )
        ),
        counts, radius,
    )


def solution(mesh):
    in_specs = (
        P("member", None, "strip", None),
        P("strip", "member"),
        P("strip", "member", None),
        P("strip", "member", None),
        P("strip", "member", None),
        P("strip", "member"),
    )
    return jax.shard_map(
        on_device, mesh=mesh, in_specs=in_specs, out_specs=P("member", None, "strip", None),
        check_vma=False,
    )
```

```python
import jax
import jax.numpy as jnp
from jax import lax
from jax.experimental import pallas as pl
from jax.experimental.pallas import tpu as pltpu
from jax.sharding import PartitionSpec as P

STEPS = 12
TURNS = 20
MEMBERS = 64
HALF = MEMBERS // 2
OWN = 4
STRIPS = 8
OWNERS = 16
ROWS = 16
COLS = 128
BLOCK = 256
OBS = 256
EDGE = 16
GUARD = 8
FIRST = GUARD + EDGE
SPAN = BLOCK + 2 * EDGE + 2 * GUARD
MESH = pl.DeviceIdType.MESH
F32 = jnp.float32
BF16 = jnp.bfloat16


def region_of(i, strip):
    y, c, z = (i // 2) % 4, i % 2, strip // 2
    a = 2 * ((y + z) % 4) + (c + y) % 2
    return a, (2 * strip + i // 8 + a % 2) % OWNERS


def owner_of(a, b):
    first = (b + OWNERS - a % 2) % OWNERS
    y = (a // 2 + 4 - first // 4) % 4
    return (first % 2) * 8 + y * 2 + (a + y) % 2, first // 2


def remote(src, dst, send, recv, where):
    return pltpu.make_async_remote_copy(
        src_ref=src, dst_ref=dst, send_sem=send, recv_sem=recv, device_id=where, device_id_type=MESH
    )


def halves(value):
    high = value.astype(BF16)
    return high, (value - high.astype(F32)).astype(BF16)


def thirds(value):
    high = value.astype(BF16)
    rest = value - high.astype(F32)
    mid = rest.astype(BF16)
    return high, mid, (rest - mid.astype(F32)).astype(BF16)


def dot(a, b):
    return jnp.dot(a, b, preferred_element_type=F32)


def matmul(a, b):
    ah, al = halves(a)
    bh, bl = halves(b)
    return dot(ah, bh) + (dot(ah, bl) + dot(al, bh))


def turn_north(value):
    return pltpu.roll(value, COLS - 1, 1)


def turn_south(value):
    return pltpu.roll(value, 1, 1)


def step_rows(src, dst, at):
    rows = pl.ds(at, 8)
    east, west = pl.ds(at + 1, 8), pl.ds(at - 1, 8)
    h, p, q = src[0, rows], src[1, rows], src[2, rows]
    he, pe, qe = src[0, east], src[1, east], src[2, east]
    hw, pw, qw = src[0, west], src[1, west], src[2, west]
    a, a2, b, b2 = 0.25 - p, 0.25 + p, 0.25 - q, 0.25 + q
    pn, ps = turn_north(p), turn_south(p)
    qn, qs = turn_north(q), turn_south(q)
    hn, hs = turn_north(h), turn_south(h)
    flow = (pe - pw) + (qn - qs)
    dst[0, rows] = (
        (he * (0.25 - pe) + hw * (0.25 + pw)) + (hn * (0.25 - qn) + hs * (0.25 + qs))
    ) - (1.0 / 64.0) * flow
    dst[1, rows] = ((a * pe + a2 * pw) + (b * pn + b2 * ps)) + (0.05 * q - (he - hw))
    dst[2, rows] = ((a * qe + a2 * qw) + (b * qn + b2 * qs)) - (0.05 * p + (hn - hs))


def kernel(
    x, cells, values, errors, count, radius, out,
    raw_cells, raw, raw_scalars, raw_radius, held, landed, work, edge, edges, halo, staged, region, mixed, packed, own, reach, near, onehot, observed, roots, mix_h, mix_l, gram,
    grams,
    load_sem, send1, recv1, send_edge, recv_edge, send2, recv2, send_obs, recv_obs, recv_reach,
    send_gram, recv_gram, send3, recv3,
):
    i = lax.axis_index("member")
    s = lax.axis_index("strip")
    a, b = region_of(i, s)
    shift = i // 8

    def neighbour(k):
        return owner_of((a + 7 + k // 3) % 8, (b + 15 + k % 3) % 16)

    to_i, to_s = owner_of(s, i)
    mine = (to_i == i) & (to_s == s)
    here = a == s
    loads = [
        pltpu.make_async_copy(cells, raw_cells, load_sem.at[0]),
        pltpu.make_async_copy(values, raw.at[0:1], load_sem.at[1]),
        pltpu.make_async_copy(errors, raw.at[1:2], load_sem.at[2]),
        pltpu.make_async_copy(count, raw_scalars, load_sem.at[3]),
        pltpu.make_async_copy(radius, raw_radius, load_sem.at[4]),
    ]
    for copy in loads:
        copy.start()
    own_input = pltpu.make_async_copy(x, held, load_sem.at[5])
    own_input.start()

    barrier = pltpu.get_barrier_semaphore()

    def greet(where):
        pl.semaphore_signal(barrier, inc=1, device_id=where, device_id_type=MESH)

    for k in range(9):
        if k != 4:
            greet(neighbour(k))
    for n in range(OWNERS):
        sender = owner_of(s, n)
        pl.when((sender[0] != i) | (sender[1] != s))(lambda sender=sender: greet(sender))
    pl.when((b != i) | (a != s))(lambda: greet((b, a)))
    for d in range(1, OWNERS):
        n = lax.rem(i + d, OWNERS)
        greet((n, ((b + OWNERS - n // 8) % OWNERS) // 2))
    for d in range(1, STRIPS):
        greet((i, lax.rem(s + d, STRIPS)))
    pl.semaphore_wait(
        barrier,
        8 + OWNERS + 1 + (OWNERS - 1) + (STRIPS - 1)
        - mine.astype(jnp.int32) - here.astype(jnp.int32),
    )

    for copy in loads:
        copy.wait()
    slots = lax.broadcasted_iota(jnp.int32, (1, OBS), 1)
    packed[0:1] = raw_cells[...].astype(F32)
    packed[1:2] = raw[0:1]
    packed[2:3] = jnp.where(slots < raw_scalars[0:1, 0:1], 1.0 / raw[1:2], 0.0)
    packed[3:4] = jnp.broadcast_to(raw_radius[0:1, 0:1].astype(F32), (1, OBS))

    @pl.when(mine)
    def _():
        pltpu.make_async_copy(packed, own, recv_obs).start()

    @pl.when(jnp.logical_not(mine))
    def _():
        remote(packed, own, send_obs.at[9], recv_obs, (to_i, to_s)).start()

    def columns_of(strip, n):
        return pl.ds(pl.multiple_of(((2 * strip + shift + n) % OWNERS) * COLS, COLS), COLS)

    strip_rows = pl.ds(pl.multiple_of(s * ROWS, ROWS), ROWS)

    def send_member(j):
        for d in range(1, STRIPS):
            to = lax.rem(s + d, STRIPS)
            for h in range(2):
                remote(
                    held.at[j, :, :, columns_of(to, h)],
                    landed.at[j, :, strip_rows, pl.ds(h * COLS, COLS)],
                    send1.at[j], recv1.at[j], (i, to),
                ).start()

    own_input.wait()
    send_member(0)
    for j in range(OWN):
        for h in range(2):
            pltpu.make_async_copy(
                x.at[j, :, :, columns_of(s, h)],
                landed.at[j, :, strip_rows, pl.ds(h * COLS, COLS)],
                recv1.at[j],
            ).start()
    lanes = lax.broadcasted_iota(jnp.int32, (ROWS, COLS), 1)

    def pack_edges(to, _):
        for f in range(3):
            joined = jnp.zeros((ROWS, COLS), F32)
            for j in range(OWN):
                both = jnp.where(
                    lanes < COLS // 2,
                    held[j, f, :, columns_of(to, 2)],
                    held[j, f, :, columns_of(to, OWNERS - 1)],
                )
                turned = pltpu.roll(both, j * 2 * EDGE + EDGE, 1)
                joined = jnp.where(lanes // (2 * EDGE) == j, turned, joined)
            edge[to, f] = joined
        return 0

    lax.fori_loop(0, STRIPS, pack_edges, 0)
    for d in range(1, STRIPS):
        to = lax.rem(s + d, STRIPS)
        remote(
            edge.at[to], edges.at[:, strip_rows], send_edge, recv_edge, (i, to)
        ).start()
    for j in range(1, OWN):
        send_member(j)
    edges[:, strip_rows] = edge[s]

    for g in range(2):
        for f in range(3):
            work[g, f, 0:GUARD] = jnp.zeros((GUARD, COLS), F32)
            work[g, f, SPAN - GUARD : SPAN] = jnp.zeros((GUARD, COLS), F32)
    ping, pong = work.at[0], work.at[1]

    def arrive(j):
        pltpu.make_async_copy(landed.at[j], landed.at[j], recv1.at[j]).wait()
        for f in range(3):
            scale = 1.0 / 64.0 if f == 0 else 0.125
            for c in range(2):
                turned = landed[j, f, :, c * COLS : (c + 1) * COLS].T * scale
                ping[f, FIRST + c * COLS : FIRST + (c + 1) * COLS] = turned

    def send_fields(j, low, high):
        for d in range(STRIPS):
            to_a = lax.rem(a + d, STRIPS)
            for e in range(2):
                n = (to_a + d + e) % 2
                src = staged.at[
                    j, low:high, pl.ds(pl.multiple_of(to_a * ROWS, ROWS), ROWS),
                    pl.ds(pl.multiple_of(n * COLS, COLS), COLS),
                ]
                dst = region.at[low:high, :, OWNERS * j + i]
                done = recv2.at[j if low == 0 else OWN]
                if d == 0 and e == 0:
                    pltpu.make_async_copy(src, dst, done).start()
                else:
                    to = owner_of(to_a, (2 * s + shift + n) % OWNERS)
                    remote(src, dst, send2, done, to).start()

    def forecast(j):
        for f in range(3):
            low, mid, high = (2 * j) * EDGE, (2 * j + 1) * EDGE, (2 * j + 2) * EDGE
            ping[f, GUARD:FIRST] = halo[f, low:mid]
            ping[f, FIRST + BLOCK : FIRST + BLOCK + EDGE] = halo[f, mid:high]

        def sweep(src, dst):
            for n in range((SPAN - 2 * GUARD) // 8):
                step_rows(src, dst, GUARD + 8 * n)

        def two_steps(n, _):
            sweep(ping, pong)
            sweep(pong, ping)
            return 0

        lax.fori_loop(0, STEPS // 2, two_steps, 0)
        for f in range(3):
            scale = 64.0 if f == 0 else 8.0
            for c in range(2):
                block = ping[f, FIRST + c * COLS : FIRST + (c + 1) * COLS]
                staged[j, f, :, c * COLS : (c + 1) * COLS] = block.T * scale
            if f == 0:
                send_fields(j, 0, 1)

    def reach_copy(k):
        return remote(
            reach, near.at[k], send_obs.at[k], recv_reach.at[k], neighbour(k)
        )

    pltpu.make_async_copy(own, own, recv_obs).wait()
    reach[...] = jnp.broadcast_to(own[3:4, :COLS], (8, COLS))
    for k in range(9):
        if k != 4:
            reach_copy(k).start()
    place = own[0:1]

    def mark(n, _):
        at = pl.multiple_of(n * COLS, COLS)
        cell = lax.broadcasted_iota(jnp.int32, (COLS, OBS), 0) + at
        onehot[pl.ds(at, COLS)] = jnp.where(cell.astype(F32) == place, 1.0, 0.0).astype(BF16)
        return 0

    lax.fori_loop(0, ROWS, mark, 0)
    arrive(0)
    rest = edges.at[:, pl.ds(0, ROWS * (STRIPS - 1))]
    remote(rest, rest, send_edge, recv_edge, (i, s)).wait_recv()
    for f in range(3):
        halo[f] = edges[f].T * (1.0 / 64.0 if f == 0 else 0.125)
    forecast(0)
    send_fields(0, 1, 3)
    arrive(1)
    forecast(1)
    send_fields(1, 1, 3)
    arrive(2)
    forecast(2)
    arrive(3)
    forecast(3)

    for j in range(OWN):
        group = slice(OWNERS * j, OWNERS * (j + 1))
        some = region.at[0, :, group]
        pltpu.make_async_copy(some, some, recv2.at[j]).wait()
        found = jnp.zeros((OWNERS, OBS), F32)
        for n in range(8):
            pair = jnp.concatenate(
                [region[0, 2 * n, group], region[0, 2 * n + 1, group]], axis=1
            )
            marks = onehot[n * OBS : (n + 1) * OBS]
            part = dot(jnp.concatenate(thirds(pair), axis=0), marks)
            found = found + (
                part[:OWNERS] + (part[OWNERS : 2 * OWNERS] + part[2 * OWNERS :])
            )
        observed[group] = found
    height = observed[...]
    mean = jnp.mean(height, axis=0, keepdims=True)
    spread = height - mean
    innovation = own[1:2] - mean
    precision = own[2:3]
    line = jnp.floor(place * (1.0 / COLS))
    row_pos = (line + 0.5) * (1.0 / ROWS) - 0.5
    col_pos = (place - line * COLS + 0.5) * (1.0 / COLS) - 0.5
    wide = jnp.concatenate([spread, jnp.zeros((COLS - MEMBERS, OBS), F32)], axis=0)
    tall = jnp.concatenate([wide[:, :COLS].T, wide[:, COLS:].T], axis=0)
    columns_h, columns_l = halves(tall)
    for k in range(9):
        if k != 4:
            reach_copy(k).wait_recv()
    near[4] = reach[...]

    def gram_copy(k):
        return remote(
            gram.at[k], grams.at[k], send_gram.at[k], recv_gram.at[k], neighbour(8 - k)
        )

    weighted_h, weighted_l, pulls = [], [], []
    for k in range(9):
        r, c = row_pos + (k // 3 - 1.0), col_pos + (k % 3 - 1.0)
        radius_k = near[k, 0:1, 0:1]
        taper = jnp.exp(-0.5 * (r * r + c * c) / (radius_k * radius_k))
        weight = taper * precision
        wh, wl = halves(spread * weight)
        weighted_h.append(wh)
        weighted_l.append(wl)
        pulls.append(innovation * weight)
    wh, wl = halves(jnp.concatenate(pulls + [jnp.zeros((7, OBS), F32)], axis=0))
    weighted_h.append(wh)
    weighted_l.append(wl)
    weighted_h = jnp.concatenate(weighted_h, axis=0)
    weighted_l = jnp.concatenate(weighted_l, axis=0)
    products = dot(weighted_h, columns_h) + (
        dot(weighted_h, columns_l) + dot(weighted_l, columns_h)
    )
    for k in range(9):
        at = k * MEMBERS
        gram[k, :HALF] = products[at : at + HALF] + pltpu.roll(
            products[at + HALF : at + MEMBERS], MEMBERS, 1
        )
        gram[k, HALF:] = jnp.broadcast_to(
            products[9 * MEMBERS + k : 9 * MEMBERS + k + 1], (8, COLS)
        )
    for k in range(9):
        if k != 4:
            gram_copy(k).start()
    send_fields(2, 1, 3)
    send_fields(3, 1, 3)
    total = gram[4]
    for k in range(9):
        if k != 4:
            gram_copy(k).wait_recv()
            total = total + grams[k]

    scale = 1.0 / (MEMBERS - 1.0)
    eye = (
        lax.broadcasted_iota(jnp.int32, (MEMBERS, MEMBERS), 0)
        == lax.broadcasted_iota(jnp.int32, (MEMBERS, MEMBERS), 1)
    ).astype(F32)
    upper = total[:HALF]
    lower = pltpu.roll(upper, MEMBERS, 1)
    normal = eye + jnp.concatenate([upper[:, :MEMBERS], lower[:, :MEMBERS]], axis=0) * scale
    frob2 = jnp.sum(jnp.sum(normal * normal, axis=1, keepdims=True), axis=0, keepdims=True)
    frob = jnp.sqrt(frob2)

    roots[0], roots[1] = normal / frob, eye

    def turn(_, carry):
        u, z = roots[0], roots[1]
        for _ in range(2):
            factor = 1.5 * eye - 0.5 * matmul(z, u)
            u, z = matmul(u, factor), matmul(factor, z)
        roots[0], roots[1] = u, z
        return carry

    lax.fori_loop(0, TURNS // 2, turn, 0)
    inverse = roots[1]
    padded = jnp.concatenate(
        [
            jnp.concatenate([inverse, jnp.zeros((MEMBERS, MEMBERS), F32)], axis=1),
            jnp.zeros((MEMBERS, COLS), F32),
        ],
        axis=0,
    )
    turned = padded.T[:MEMBERS, :MEMBERS]
    pull = matmul(matmul(total[HALF:, :MEMBERS], turned), turned) / frob
    weights_h, weights_l = halves(turned / jnp.sqrt(frob) + pull[0:1] * scale)
    mix_h[...], mix_l[...] = weights_h, weights_l

    columns = pl.ds(pl.multiple_of(b * COLS, COLS), COLS)
    flows = region.at[1:3]
    for f in range(3):
        if f == 1:
            pltpu.make_async_copy(flows, flows, recv2.at[OWN]).wait()

        def rows_of(n, _):
            pair = jnp.concatenate([region[f, 2 * n], region[f, 2 * n + 1]], axis=1)
            centre = jnp.mean(pair, axis=0, keepdims=True)
            dev_h, dev_l = halves(pair - centre)
            result = centre + (
                dot(mix_h[...], dev_h)
                + (dot(mix_h[...], dev_l) + dot(mix_l[...], dev_h))
            )
            mixed[f, 2 * n] = result[:, :COLS]
            mixed[f, 2 * n + 1] = result[:, COLS:]
            return 0

        lax.fori_loop(0, ROWS // 2, rows_of, 0)
        if f == 1:
            continue
        low, high = (0, 1) if f == 0 else (1, 3)
        for d in range(OWNERS):
            to = lax.rem(i + d, OWNERS)
            for j in range(OWN):
                src = mixed.at[low:high, :, OWNERS * j + to]
                dst = out.at[j, low:high, :, columns]
                if d == 0:
                    pl.when(here)(
                        lambda src=src, dst=dst: pltpu.make_async_copy(
                            src, dst, recv3
                        ).start()
                    )
                    pl.when(jnp.logical_not(here))(
                        lambda src=src, dst=dst: remote(
                            src, dst, send3.at[1], recv3, (i, a)
                        ).start()
                    )
                else:
                    remote(src, dst, send3.at[0], recv3, (to, a)).start()

    for j in range(OWN):
        rest = landed.at[j, :, pl.ds(0, ROWS * (STRIPS - 1))]
        remote(rest, rest, send1.at[j], recv1.at[j], (i, s)).wait_send()
    rest = edges.at[:, pl.ds(0, ROWS * (STRIPS - 1))]
    remote(rest, rest, send_edge, recv_edge, (i, s)).wait_send()
    pl.when(jnp.logical_not(mine))(
        lambda: remote(packed, own, send_obs.at[9], recv_obs, (i, s)).wait_send()
    )
    for k in range(9):
        if k != 4:
            reach_copy(k).wait_send()
    rest = region.at[:, :, pl.ds(0, OWN * (OWNERS - 1))]
    remote(rest, rest, send2, recv2.at[0], (i, s)).wait_send()
    for k in range(9):
        if k != 4:
            gram_copy(k).wait_send()
    remote(rest, rest, send3.at[0], recv3, (i, s)).wait_send()
    few = region.at[:, :, pl.ds(0, OWN)]
    pl.when(jnp.logical_not(here))(
        lambda: remote(few, few, send3.at[1], recv3, (i, s)).wait_send()
    )
    remote(out, out, send3.at[0], recv3, (i, s)).wait_recv()


def on_device(fields, counts, cells, values, errors, radius):
    hbm = pl.BlockSpec(memory_space=pltpu.HBM)
    dma = pltpu.SemaphoreType.DMA
    return pl.pallas_call(
        kernel,
        out_shape=jax.ShapeDtypeStruct(fields.shape, F32),
        in_specs=[hbm] * 6,
        out_specs=pl.BlockSpec(memory_space=pl.ANY),
        scratch_shapes=[
            pltpu.VMEM((1, OBS), jnp.int32),
            pltpu.VMEM((2, OBS), F32),
            pltpu.VMEM((1, 1), jnp.int32),
            pltpu.VMEM((1, 1), jnp.int32),
            pltpu.VMEM((OWN, 3, ROWS, 2048), F32),
            pltpu.VMEM((OWN, 3, STRIPS * ROWS, BLOCK), F32),
            pltpu.VMEM((2, 3, SPAN, COLS), F32),
            pltpu.VMEM((STRIPS, 3, ROWS, COLS), F32),
            pltpu.VMEM((3, STRIPS * ROWS, COLS), F32),
            pltpu.VMEM((3, STRIPS * ROWS, COLS), F32),
            pltpu.VMEM((OWN, 3, STRIPS * ROWS, BLOCK), F32),
            pltpu.VMEM((3, ROWS, MEMBERS, COLS), F32),
            pltpu.VMEM((3, ROWS, MEMBERS, COLS), F32),
            pltpu.VMEM((8, OBS), F32),
            pltpu.VMEM((8, OBS), F32),
            pltpu.VMEM((8, COLS), F32),
            pltpu.VMEM((9, 8, COLS), F32),
            pltpu.VMEM((ROWS * COLS, OBS), BF16),
            pltpu.VMEM((MEMBERS, OBS), F32),
            pltpu.VMEM((2, MEMBERS, MEMBERS), F32),
            pltpu.VMEM((MEMBERS, MEMBERS), BF16),
            pltpu.VMEM((MEMBERS, MEMBERS), BF16),
            pltpu.VMEM((9, HALF + 8, COLS), F32),
            pltpu.VMEM((9, HALF + 8, COLS), F32),
            dma((6,)), dma((OWN,)), dma((OWN,)), dma, dma, dma, dma((OWN + 1,)),
            dma((10,)), dma, dma((9,)),
            dma((9,)), dma((9,)), dma((2,)), dma,
        ],
        compiler_params=pltpu.CompilerParams(
            collective_id=0, has_side_effects=True, vmem_limit_bytes=40 * 1024 * 1024
        ),
        name="forecast_and_analysis",
    )(
        *(
            pltpu.with_memory_space_constraint(operand, pltpu.HBM)
            for operand in (
                fields, cells.reshape(1, OBS), values.reshape(1, OBS), errors.reshape(1, OBS),
            )
        ),
        counts, radius,
    )


def solution(mesh):
    in_specs = (
        P("member", None, "strip", None),
        P("strip", "member"),
        P("strip", "member", None),
        P("strip", "member", None),
        P("strip", "member", None),
        P("strip", "member"),
    )
    return jax.shard_map(
        on_device, mesh=mesh, in_specs=in_specs, out_specs=P("member", None, "strip", None),
        check_vma=False,
    )
```
